32 devices in a mesh: dp: 8 (over z, core), tensor: 4 (over y, x).
Axes of the slice: x: 2, y: 2, z: 4, core: 2. Of those that a mesh axis runs over, the one named last changes fastest.
Arguments:
- latents: bfloat16 [88, 256, 640], P('dp', 'tensor'), may hold values from -6 to 6
- cotangent: bfloat16 [88, 256, 640], P('dp', 'tensor'), may hold values from -6 to 6
- trunc_steps: int32 [8], replicated, may hold values from 30 to 40, as said below
- timesteps: int32 [88], replicated, may hold values from 100 to 900
- tile_map: int32 [88], replicated, may hold values from 0 to 87, as said below
- gain: float32 [640], replicated, may hold values from 0.5 to 1.5
- w_value: bfloat16 [640, 2560], P(None, 'tensor'), may hold values from -0.25 to 0.25
- w_gate: bfloat16 [640, 2560], P(None, 'tensor'), may hold values from -0.25 to 0.25
- w_out: bfloat16 [640, 2560], P(None, 'tensor'), may hold values from -0.125 to 0.125
Outputs:
- placed_grad: bfloat16 [88, 256, 640], P('dp', 'tensor')
- grad_value: float32 [640, 2560], P('dp', 'tensor')
- grad_gate: float32 [640, 2560], P('dp', 'tensor')
- grad_out_proj: float32 [640, 2560], P('dp', 'tensor')
- grad_gain: float32 [640], replicated
The draws below stay inside these ranges and needn't reach their ends.
Inputs may be any that keep to these rules, and one draw needn't show every extreme that they name: trunc_steps lies in 30 to 40, so a prompt has 1 to 11 live slots, its lowest ones. tile_map is a permutation of 0 to 87. Output slots g * 11 to g * 11 + 10 form group g; the live items go to the lowest slots of the groups, and each group receives the floor or the ceiling of (number of live items) / 8 of them.
All inputs are finite; a program needn't handle non-finite values.
Results may differ from the reference program's by a relative error of at most 0.0068.
Values may be sent and summed in bfloat16 or wider, within the bound.
A program may use at most 64 MiB of HBM per device.

```python
import jax
import jax.numpy as jnp
from jax import lax

C = 640
FI = 2560
ROWS = 256
SLOTS = 11
PROMPTS = 8
ITEMS = 88


def chain_plan(key):
    steps = jax.random.randint(jax.random.fold_in(key, 11), (PROMPTS,), 30, 41).astype(jnp.int32)
    item_ids = jnp.arange(ITEMS, dtype=jnp.int32)
    live = (item_ids % SLOTS < jnp.repeat(steps, SLOTS) - 29).astype(jnp.int32)
    shuffled = jax.random.permutation(jax.random.fold_in(key, 12), ITEMS).astype(jnp.int32)
    ranking = (1 - live) * ITEMS + shuffled
    ordering = jnp.argsort(ranking, stable=True).astype(jnp.int32)
    groups = ITEMS // SLOTS
    slot_of = item_ids % groups * SLOTS + item_ids // groups
    tile_map = jnp.zeros((ITEMS,), jnp.int32).at[ordering].set(slot_of.astype(jnp.int32))
    return (steps, tile_map)


def draw_trunc_steps(key, part):
    return chain_plan(key)[0]


def draw_tile_map(key, part):
    return chain_plan(key)[1]


def with_ends(result, own_key, low, top_value):
    longest = result.shape.index(max(result.shape))
    spots = []
    for shift in (0, 1):
        where = [jax.random.randint(jax.random.fold_in(own_key, axis), (), 0, length) for axis, length in enumerate(result.shape)]
        where[longest] = (where[longest] + shift) % result.shape[longest]
        spots.append(tuple(where))
    return result.at[spots[0]].set(low).at[spots[1]].set(top_value)


def block_scale(rng, extent, cuts, low, high):
    def one(dim, parts):
        draws = jax.random.uniform(jax.random.fold_in(jax.random.fold_in(rng, 6), dim), (parts,), jnp.float32, low / len(cuts), high / len(cuts))
        return jnp.repeat(jnp.exp(draws), extent[dim] // parts).reshape((-1,) + (1,) * (len(extent) - dim - 1))

    level = one(*cuts[0])
    for cut in cuts[1:]:
        level = level * one(*cut)
    return level


def bell_draw(stream_key, dims, scale, reach, cuts=(), held_as=jnp.bfloat16):
    drawn = scale * jax.random.normal(stream_key, dims, jnp.float32)
    if cuts:
        drawn = drawn * block_scale(stream_key, dims, cuts, -0.22, 0.18)
    return jnp.clip(drawn, -reach, reach).astype(held_as)


def setup_inputs(seed: int = 0) -> dict:
    key_of = jax.random.split(jax.random.key(seed), 10)
    return {
        "latents": bell_draw(key_of[0], (ITEMS, ROWS, C), 1.0, 6.0, ((0, 8), (1, 4))),
        "cotangent": bell_draw(key_of[1], (ITEMS, ROWS, C), 1.0, 6.0, ((0, 8), (1, 4))),
        "trunc_steps": draw_trunc_steps(jax.random.fold_in(key_of[9], 71), 0),
        "timesteps": with_ends(jax.random.randint(key_of[3], (ITEMS,), 100, 901), jax.random.fold_in(key_of[3], 1), 100, 900).astype(jnp.int32),
        "tile_map": draw_tile_map(jax.random.fold_in(key_of[9], 71), 0),
        "gain": jnp.clip(1.0 + 0.1 * jax.random.normal(key_of[5], (C,), jnp.float32), 0.5, 1.5),
        "w_value": bell_draw(key_of[6], (C, FI), C ** -0.5, 0.25, ((1, 4),)),
        "w_gate": bell_draw(key_of[7], (C, FI), C ** -0.5, 0.25, ((1, 4),)),
        "w_out": bell_draw(key_of[8], (C, FI), FI ** -0.5, 0.125, ((1, 4),)),
    }


eps = 1e-05

def alpha_bars():
    betas = jnp.linspace(0.00085 ** 0.5, 0.012 ** 0.5, 1000, dtype=jnp.float32) ** 2
    return jnp.exp(jnp.cumsum(jnp.log1p(-betas)))

def gelu_parts(inputs):
    cdf = 0.5 * (1.0 + lax.erf(inputs * 0.7071067811865476))
    density = jnp.exp(-0.5 * inputs * inputs) * 0.3989422804014327
    return (inputs * cdf, cdf + inputs * density)

def item_backward(normed, grad_tile, w_value, w_gate, w_out):
    values_proj = jnp.dot(normed, w_value, preferred_element_type=jnp.float32)
    gate_proj = jnp.dot(normed, w_gate, preferred_element_type=jnp.float32)
    gelu_gate, gelu_slope = gelu_parts(gate_proj)
    hidden = (values_proj * gelu_gate).astype(jnp.bfloat16)
    d_hidden = jnp.dot(grad_tile, w_out, preferred_element_type=jnp.float32)
    d_value = (d_hidden * gelu_gate).astype(jnp.bfloat16)
    d_gate = (d_hidden * values_proj * gelu_slope).astype(jnp.bfloat16)
    first_dims = (((0,), (0,)), ((), ()))
    last_dims = (((1,), (1,)), ((), ()))
    grad_wv = lax.dot_general(normed, d_value, first_dims, preferred_element_type=jnp.float32)
    grad_wg = lax.dot_general(normed, d_gate, first_dims, preferred_element_type=jnp.float32)
    grad_wo = lax.dot_general(grad_tile, hidden, first_dims, preferred_element_type=jnp.float32)
    d_normed = lax.dot_general(d_value, w_value, last_dims, preferred_element_type=jnp.float32)
    d_normed = d_normed + lax.dot_general(d_gate, w_gate, last_dims, preferred_element_type=jnp.float32)
    return (grad_wv, grad_wg, grad_wo, d_normed)

def reference(latents, cotangent, trunc_steps, timesteps, tile_map, gain, w_value, w_gate, w_out):
    total = latents.shape[0]
    item_ids = jnp.arange(total, dtype=jnp.int32)
    live = item_ids % SLOTS < jnp.repeat(trunc_steps, SLOTS) - 29
    noise_scale = jnp.sqrt(1.0 - alpha_bars()[timesteps])
    width = latents.shape[2]
    inner = w_value.shape[1]

    def one_item(carry, inputs):
        tile, cot_tile, item_scale, is_live = inputs
        x_float = tile.astype(jnp.float32)
        row_mean = lax.optimization_barrier(jnp.mean(x_float, axis=-1, keepdims=True))
        centred = x_float - row_mean
        row_var = lax.optimization_barrier(jnp.mean(centred * centred, axis=-1, keepdims=True))
        inv_std = lax.rsqrt(row_var + eps)
        x_hat = centred * inv_std
        normed = (x_hat * gain).astype(jnp.bfloat16)
        grad_tile = (cot_tile.astype(jnp.float32) * item_scale).astype(jnp.bfloat16)

        def run(unused):
            grad_wv, grad_wg, grad_wo, d_normed = item_backward(normed, grad_tile, w_value, w_gate, w_out)
            d_hat = d_normed * gain
            input_grad = grad_tile.astype(jnp.float32) + inv_std * (d_hat - lax.optimization_barrier(jnp.mean(d_hat, axis=-1, keepdims=True)) - x_hat * lax.optimization_barrier(jnp.mean(d_hat * x_hat, axis=-1, keepdims=True)))
            gain_part = lax.optimization_barrier(jnp.sum(d_normed * x_hat, axis=0))
            return (grad_wv, grad_wg, grad_wo, gain_part, input_grad.astype(jnp.bfloat16))

        def skip(unused):
            zero_w = jnp.zeros((width, inner), jnp.float32)
            return (zero_w, zero_w, zero_w, jnp.zeros((width,), jnp.float32), jnp.zeros(tile.shape, jnp.bfloat16))
        grad_wv, grad_wg, grad_wo, gain_part, input_grad = lax.cond(is_live, run, skip, None)
        carry = (carry[0] + grad_wv, carry[1] + grad_wg, carry[2] + grad_wo, carry[3] + gain_part)
        return (carry, input_grad)
    zero_w = jnp.zeros((width, inner), jnp.float32)
    init = (zero_w, zero_w, zero_w, jnp.zeros((width,), jnp.float32))
    sums, input_grads = lax.scan(one_item, init, (latents, cotangent, noise_scale, live))
    placed_grad = jnp.zeros(latents.shape, jnp.bfloat16).at[tile_map.astype(jnp.int32)].set(input_grads)
    return (placed_grad, sums[0], sums[1], sums[2], sums[3])
```

```python
import functools

import jax
import jax.numpy as jnp
import numpy as np
from jax import lax
from jax.experimental import pallas as pl
from jax.experimental.pallas import tpu as pltpu
from jax.sharding import PartitionSpec as P

eps = 1e-05


def noise_table():
    betas = np.linspace(0.00085**0.5, 0.012**0.5, 1000) ** 2
    abar = np.exp(np.cumsum(np.log1p(-betas)))
    return np.sqrt(1.0 - abar).astype(np.float32)


def block_kernel(n, groups, rounds, ahead, steps_ref, times_ref, map_ref, table_ref, x_ref, cot_ref,
                 gain_ref, wv_ref, wg_ref, wo_ref, ig_ref, gg_ref, dv_ref, dg_ref, do_ref,
                 full, part_a, part_b, in_a, in_b, sum_a, sum_b, last_a, last_b, held,
                 acc_v, acc_g, acc_o, placed, gain_one, gain_two,
                 dw_part, dw_pair, dw_sum, dw_down, dw_up, pool, scale_ref, source_ref, keep_ref,
                 ag_send, ag_recv, sa_send, sa_recv, sb_send, sb_recv, ta_send, ta_recv,
                 tb_send, tb_recv, out_send, out_recv, gain_send, gain_recv, far_send, far_recv,
                 pair_send, pair_recv, down_send, down_recv, up_send, up_recv,
                 pool_send, pool_recv):
    slots, rows, width = x_ref.shape
    half = rows // 2
    extra = slots - rounds
    me = lax.axis_index("tensor")
    high = n // 2
    my_high, my_low = me // 2, me % 2
    pair = my_high * 2 + (1 - my_low)
    line_high = [(my_high + k) % high for k in range(1, high)]
    line = [h * 2 + my_low for h in line_high]
    peers = [(me + k) % n for k in range(1, n)]
    first = (((0,), (0,)), ((), ()))
    last = (((1,), (1,)), ((), ()))
    group = lax.axis_index("dp")
    chips = groups // 2
    chip, core = group // 2, group % 2
    twin = chip * 2 + (1 - core)
    block = dw_part.shape[2]
    own_live = jnp.clip(steps_ref[group] - 29, 1, slots)
    twin_live = jnp.clip(steps_ref[twin] - 29, 1, slots)

    def cross(src, dst, send_sem, recv_sem, peer):
        return pltpu.make_async_remote_copy(
            src_ref=src, dst_ref=dst, send_sem=send_sem, recv_sem=recv_sem,
            device_id={"dp": peer}, device_id_type=pl.DeviceIdType.MESH,
        )

    def send(src, dst, send_sem, recv_sem, peer):
        return pltpu.make_async_remote_copy(
            src_ref=src, dst_ref=dst, send_sem=send_sem, recv_sem=recv_sem,
            device_id={"tensor": peer}, device_id_type=pl.DeviceIdType.MESH,
        )

    def out_copy(t, owner, index, peer):
        spot = placed.at[owner * rounds + t]
        return cross(spot, spot, out_send.at[t, index], out_recv.at[t, owner], peer)

    def own_outs(t, act):
        @pl.when(chip + 1 < chips)
        def _():
            act(out_copy(t, group, 0, group + 2))

        @pl.when(chip >= 1)
        def _():
            act(out_copy(t, group, 1, group - 2))

        act(out_copy(t, group, 2, twin))

    def relay_outs(t, d, act, arrive):
        base = 3 + 4 * (d - 1)

        @pl.when(chip >= d)
        def _():
            owner = group - 2 * d
            if arrive:
                out_copy(t, owner, base, twin).wait_recv()

            @pl.when(chip + 1 < chips)
            def _():
                act(out_copy(t, owner, base, group + 2))

            act(out_copy(t, owner, base + 1, twin))

        @pl.when(chip + d < chips)
        def _():
            owner = group + 2 * d
            if arrive:
                out_copy(t, owner, base + 2, twin).wait_recv()

            @pl.when(chip >= 1)
            def _():
                act(out_copy(t, owner, base + 2, group - 2))

            act(out_copy(t, owner, base + 3, twin))

    def begin(copy):
        copy.start()

    def done(copy):
        copy.wait_send()

    def own_copies(t):
        found = []
        for peer in [pair] + line:
            for kind in (0, 1):
                found.append(send(
                    full.at[t, kind, me], full.at[t, kind, me],
                    ag_send.at[t, len(found)], ag_recv.at[t, kind, me], peer,
                ))
        return found

    def passed_copies(t):
        found = []
        base = 2 * high
        for peer in line:
            found.append(send(
                full.at[t, 0, pair], full.at[t, 0, pair],
                ag_send.at[t, base + len(found)], ag_recv.at[t, 0, pair], peer,
            ))
        for owner in line:
            found.append(send(
                full.at[t, 1, owner], full.at[t, 1, owner],
                ag_send.at[t, base + len(found)], ag_recv.at[t, 1, owner], pair,
            ))
        return found

    def arrived(t, kind, owner):
        send(full.at[t, kind, owner], full.at[t, kind, owner], ag_send.at[t, 0],
             ag_recv.at[t, kind, owner], pair).wait_recv()

    def one_a(t):
        return [send(part_a.at[t, 1 - my_low], in_a.at[t], sa_send.at[t], sa_recv.at[t], pair)]

    def one_b(t):
        return [
            send(part_b.at[t, h], in_b.at[t, k], sb_send.at[t, k], sb_recv.at[t, k], p)
            for k, (h, p) in enumerate(zip(line_high, line, strict=True))
        ]

    def two_a(t):
        return [
            send(sum_a.at[t, k], last_a.at[t, k], ta_send.at[t, k], ta_recv.at[t, k], p)
            for k, p in enumerate(line)
        ]

    def two_b(t):
        return [send(sum_b.at[t], last_b.at[t], tb_send.at[t], tb_recv.at[t], pair)]

    def pick(values, index):
        found = values[0]
        for k in range(1, len(values)):
            found = jnp.where(index == k, values[k], found)
        return found

    def start_own(t):
        for copy in own_copies(t):
            copy.start()

    def pass_on(t):
        for owner in [pair] + line:
            for kind in (0, 1):
                arrived(t, kind, owner)
        for copy in passed_copies(t):
            copy.start()

    barrier = pltpu.get_barrier_semaphore()
    for peer in peers:
        pl.semaphore_signal(
            barrier, inc=1, device_id={"tensor": peer}, device_id_type=pl.DeviceIdType.MESH
        )
    for k in range(1, groups):
        pl.semaphore_signal(
            barrier, inc=1, device_id={"dp": (group + k) % groups},
            device_id_type=pl.DeviceIdType.MESH,
        )
    for kind, ref in enumerate((x_ref, cot_ref)):
        full[0, kind, me] = ref[0]
    pl.semaphore_wait(barrier, n - 1 + groups - 1)
    pool_copies = [
        cross(ref.at[pl.ds(rounds, extra)], pool.at[kind], pool_send.at[kind], pool_recv.at[kind],
              twin)
        for kind, ref in enumerate((x_ref, cot_ref)) if extra
    ]
    start_own(0)
    for copy in pool_copies:
        copy.start()
    for copy in pool_copies:
        copy.wait()

    def fill(t, carry):
        for kind, ref in enumerate((x_ref, cot_ref)):
            tile = ref[t]
            if extra:
                spare = pool[kind, jnp.clip(t - own_live, 0, extra - 1)]
                tile = jnp.where(t < own_live, tile, spare)
            full[t, kind, me] = tile
        return carry

    lax.fori_loop(1, rounds, fill, 0)
    for t in range(1, min(ahead, rounds)):
        start_own(t)

    def set_scale(t, carry):
        mine = t < own_live
        item = jnp.where(mine, group * slots + t, twin * slots + rounds + t - own_live)
        item = jnp.clip(item, 0, groups * slots - 1)
        alive = jnp.logical_or(mine, rounds + t - own_live < twin_live)
        scale_ref[t] = jnp.where(alive, table_ref[times_ref[item]], 0.0)
        return carry

    lax.fori_loop(0, rounds, set_scale, 0)

    def invert(i, found):
        spot = map_ref[i] - group * slots
        return tuple(jnp.where(spot == s, i, item) for s, item in enumerate(found))

    items = lax.fori_loop(0, groups * slots, invert, tuple(jnp.int32(0) for _ in range(slots)))
    for s, item in enumerate(items):
        owner = item // slots
        index = item % slots
        live = jnp.clip(steps_ref[owner] - 29, 1, slots)
        other = owner + 1 - 2 * (owner % 2)
        other_live = jnp.clip(steps_ref[other] - 29, 1, slots)
        spot = jnp.where(
            index < rounds, owner * rounds + index, other * rounds + other_live + index - rounds
        )
        source_ref[s] = jnp.clip(spot, 0, groups * rounds - 1)
        keep_ref[s] = jnp.where(index < live, 1.0, 0.0)

    acc_v[...] = jnp.zeros_like(acc_v)
    acc_g[...] = jnp.zeros_like(acc_g)
    acc_o[...] = jnp.zeros_like(acc_o)
    gg_ref[...] = jnp.zeros_like(gg_ref)
    gain = gain_ref[...].reshape(1, width)
    pass_on(0)

    def combine(t):
        for copy in one_a(t):
            copy.wait_recv()
        sums = []
        for h in range(high):
            mine = pick([part_a[t, l, h] for l in range(2)], my_low)
            sums.append(mine.astype(jnp.float32) + in_a[t, h].astype(jnp.float32))
        for k, h in enumerate(line_high):
            sum_a[t, k] = pick(sums, h).astype(jnp.bfloat16)
        for copy in two_a(t):
            copy.start()
        held[t, 0] = pick(sums, my_high)
        for copy in one_b(t):
            copy.wait_recv()
        sums = []
        for l in range(2):
            both = pick([part_b[t, h, l] for h in range(high)], my_high).astype(jnp.float32)
            for k in range(high - 1):
                both += in_b[t, k, l].astype(jnp.float32)
            sums.append(both)
        sum_b[t] = pick(sums, 1 - my_low).astype(jnp.bfloat16)
        for copy in two_b(t):
            copy.start()
        held[t, 1] = pick(sums, my_low)

    def finish(t):
        top = held[t, 0]
        low = held[t, 1]
        for k, copy in enumerate(two_a(t)):
            copy.wait_recv()
            top += last_a[t, k].astype(jnp.float32)
        for copy in two_b(t):
            copy.wait_recv()
        low += last_b[t].astype(jnp.float32)
        d_normed = jnp.concatenate([top, low], axis=0)
        x = full[t, 0, me].astype(jnp.float32)
        centred = x - jnp.mean(x, axis=-1, keepdims=True)
        inv_std = lax.rsqrt(jnp.mean(centred * centred, axis=-1, keepdims=True) + eps)
        x_hat = centred * inv_std
        grad = (full[t, 1, me].astype(jnp.float32) * scale_ref[t]).astype(jnp.bfloat16)
        d_hat = d_normed * gain
        placed[group * rounds + t] = (grad.astype(jnp.float32) + inv_std * (
            d_hat
            - jnp.mean(d_hat, axis=-1, keepdims=True)
            - x_hat * jnp.mean(d_hat * x_hat, axis=-1, keepdims=True)
        )).astype(jnp.bfloat16)
        own_outs(t, begin)
        gg_ref[...] += jnp.sum(d_normed * x_hat, axis=0, keepdims=True)

    def after(t):
        @pl.when(t >= 1)
        def _():
            combine(t - 1)

        @pl.when(t >= 2)
        def _():
            finish(t - 2)

        for d in range(1, chips):
            @pl.when(t >= 2 + d)
            def _():
                relay_outs(t - 2 - d, d, begin, True)

    def relay_left(t):
        for d in range(1, chips):
            if 0 <= t - 2 - d < rounds:
                relay_outs(t - 2 - d, d, begin, True)

    def one_tile(t, carry):
        @pl.when(t + ahead < rounds)
        def _():
            start_own(t + ahead)

        @pl.when(t + 1 < rounds)
        def _():
            pass_on(t + 1)

        far = [h * 2 + (1 - my_low) for h in line_high]
        for owner in far:
            for kind in (0, 1):
                arrived(t, kind, owner)
        x = full[t, 0].reshape(n * rows, width).astype(jnp.float32)
        centred = x - jnp.mean(x, axis=-1, keepdims=True)
        inv_std = lax.rsqrt(jnp.mean(centred * centred, axis=-1, keepdims=True) + eps)
        normed = (centred * inv_std * gain).astype(jnp.bfloat16)
        cot = full[t, 1].reshape(n * rows, width).astype(jnp.float32)
        grad = (cot * scale_ref[t]).astype(jnp.bfloat16)
        values = jnp.dot(normed, wv_ref[...], preferred_element_type=jnp.float32)
        gate = jnp.dot(normed, wg_ref[...], preferred_element_type=jnp.float32)
        d_hidden = jnp.dot(grad, wo_ref[...], preferred_element_type=jnp.float32)
        cdf = 0.5 * (1.0 + lax.erf(gate * 0.7071067811865476))
        density = jnp.exp(-0.5 * gate * gate) * 0.3989422804014327
        gelu = gate * cdf
        hidden = (values * gelu).astype(jnp.bfloat16)
        d_value = (d_hidden * gelu).astype(jnp.bfloat16)
        d_gate = (d_hidden * values * (cdf + gate * density)).astype(jnp.bfloat16)
        d_normed = lax.dot_general(d_value, wv_ref[...], last, preferred_element_type=jnp.float32)
        d_normed += lax.dot_general(d_gate, wg_ref[...], last, preferred_element_type=jnp.float32)
        d_normed = d_normed.astype(jnp.bfloat16).reshape(n, rows, width)
        for h in range(high):
            for l in range(2):
                part_a[t, l, h] = d_normed[h * 2 + l, :half]
                part_b[t, h, l] = d_normed[h * 2 + l, half:]
        for copy in one_a(t) + one_b(t):
            copy.start()
        acc_v[...] += lax.dot_general(normed, d_value, first, preferred_element_type=jnp.float32)
        acc_g[...] += lax.dot_general(normed, d_gate, first, preferred_element_type=jnp.float32)
        acc_o[...] += lax.dot_general(grad, hidden, first, preferred_element_type=jnp.float32)
        after(t)
        return carry

    lax.fori_loop(0, rounds, one_tile, 0)
    for d in range(groups):
        rows_of = slice(d * block, (d + 1) * block)
        for k, acc in enumerate((acc_v, acc_g, acc_o)):
            dw_part[d, k] = acc[rows_of, :].astype(jnp.bfloat16)
    pair_copies = [
        cross(dw_part.at[c * 2 + 1 - core], dw_pair.at[c], pair_send.at[c], pair_recv.at[c], twin)
        for c in range(chips)
    ]
    for copy in pair_copies:
        copy.start()

    combine(rounds - 1)
    for t in (rounds, rounds + 1):
        if t >= 2:
            finish(t - 2)
        relay_left(t)
    gain_one[me] = gg_ref[...]
    gain_copies = [
        send(gg_ref, gain_one.at[me], gain_send.at[k], gain_recv.at[me], peer)
        for k, peer in enumerate(peers)
    ]
    for copy in gain_copies:
        copy.start()
    for copy in pair_copies:
        copy.wait()
    for c in range(chips):
        both = dw_part[c * 2 + core].astype(jnp.float32) + dw_pair[c].astype(jnp.float32)
        dw_sum[c] = both.astype(jnp.bfloat16)

    def down_copy(c, k):
        return cross(dw_sum.at[c, k], dw_down.at[c, k], down_send.at[c, k], down_recv.at[c, k],
                     group - 2)

    def up_copy(c, k):
        return cross(dw_sum.at[c, k], dw_up.at[c, k], up_send.at[c, k], up_recv.at[c, k], group + 2)

    def move(j, k):
        @pl.when(chip > j)
        def _():
            @pl.when(chip + 1 < chips)
            def _():
                down_copy(j, k).wait_recv()
                both = dw_sum[j, k].astype(jnp.float32) + dw_down[j, k].astype(jnp.float32)
                dw_sum[j, k] = both.astype(jnp.bfloat16)

            down_copy(j, k).start()

        c = chips - 1 - j

        @pl.when(chip < c)
        def _():
            @pl.when(chip >= 1)
            def _():
                up_copy(c, k).wait_recv()
                both = dw_sum[c, k].astype(jnp.float32) + dw_up[c, k].astype(jnp.float32)
                dw_sum[c, k] = both.astype(jnp.bfloat16)

            up_copy(c, k).start()

    for j in range(chips - 1):
        for k in range(3):
            move(j, k)
    for t in range(rounds + 2, rounds + 1 + chips):
        relay_left(t)
    for peer in peers:
        send(gg_ref, gain_one.at[peer], gain_send.at[0], gain_recv.at[peer], peer).wait_recv()
    for copy in gain_copies:
        copy.wait_send()
    gain_sum = gain_one[0]
    for k in range(1, n):
        gain_sum += gain_one[k]
    gain_two[group] = gain_sum
    far_copies = [
        cross(gain_two.at[group], gain_two.at[group], far_send.at[k], far_recv.at[group],
              (group + k) % groups)
        for k in range(1, groups)
    ]
    for copy in far_copies:
        copy.start()

    def settle(t, carry):
        for c in range(chips):
            out_copy(t, c * 2 + 1 - core, 0, twin).wait_recv()
        for copy in (own_copies(t) + passed_copies(t) + one_a(t) + one_b(t) + two_a(t) + two_b(t)):
            copy.wait_send()
        own_outs(t, done)
        for d in range(1, chips):
            relay_outs(t, d, done, False)
        return carry

    lax.fori_loop(0, rounds, settle, 0)

    def place(t, carry):
        ig_ref[t] = (placed[source_ref[t]].astype(jnp.float32) * keep_ref[t]).astype(jnp.bfloat16)
        return carry

    lax.fori_loop(0, slots, place, 0)
    for k in range(1, groups):
        peer = (group + k) % groups
        cross(gain_two.at[peer], gain_two.at[peer], far_send.at[k], far_recv.at[peer],
              peer).wait_recv()
    for copy in far_copies:
        copy.wait_send()
    gain_total = gain_two[0]
    for k in range(1, groups):
        gain_total += gain_two[k]
    gg_ref[...] = gain_total
    outs = (dv_ref, dg_ref, do_ref)
    for c in range(chips):
        @pl.when(chip == c)
        def _():
            for k, ref in enumerate(outs):
                total = dw_sum[c, k].astype(jnp.float32)
                if c + 1 < chips:
                    down_copy(c, k).wait_recv()
                    total += dw_down[c, k].astype(jnp.float32)
                if c >= 1:
                    up_copy(c, k).wait_recv()
                    total += dw_up[c, k].astype(jnp.float32)
                ref[...] = total

    for j in range(chips - 1):
        for k in range(3):
            @pl.when(chip > j)
            def _():
                down_copy(j, k).wait_send()

            @pl.when(chip < chips - 1 - j)
            def _():
                up_copy(chips - 1 - j, k).wait_send()


def block_backward(n, groups, rounds, ident, steps, times, tile_map, table, x, cot, gain,
                   w_value, w_gate, w_out):
    slots, rows, width = x.shape
    inner = w_value.shape[1]
    chips = groups // 2
    high = n // 2
    half = rows // 2
    others = max(high - 1, 1)
    block = width // groups
    vmem = pl.BlockSpec(memory_space=pltpu.VMEM)
    smem = pl.BlockSpec(memory_space=pltpu.SMEM)
    grads = jax.ShapeDtypeStruct((block, inner), jnp.float32)
    dma = pltpu.SemaphoreType.DMA
    bf16 = jnp.bfloat16
    return pl.pallas_call(
        functools.partial(block_kernel, n, groups, rounds, 3),
        in_specs=[smem] * 4 + [vmem] * 6,
        out_specs=[vmem] * 5,
        out_shape=[
            jax.ShapeDtypeStruct((slots, rows, width), bf16),
            jax.ShapeDtypeStruct((1, width), jnp.float32),
            grads,
            grads,
            grads,
        ],
        scratch_shapes=[
            pltpu.VMEM((rounds, 2, n, rows, width), bf16),
            pltpu.VMEM((rounds, 2, high, half, width), bf16),
            pltpu.VMEM((rounds, high, 2, half, width), bf16),
            pltpu.VMEM((rounds, high, half, width), bf16),
            pltpu.VMEM((rounds, others, 2, half, width), bf16),
            pltpu.VMEM((rounds, others, half, width), bf16),
            pltpu.VMEM((rounds, half, width), bf16),
            pltpu.VMEM((rounds, others, half, width), bf16),
            pltpu.VMEM((rounds, half, width), bf16),
            pltpu.VMEM((rounds, 2, half, width), jnp.float32),
        ]
        + [pltpu.VMEM((width, inner), jnp.float32)] * 3
        + [
            pltpu.VMEM((groups * rounds, rows, width), bf16),
            pltpu.VMEM((n, 1, width), jnp.float32),
            pltpu.VMEM((groups, 1, width), jnp.float32),
            pltpu.VMEM((groups, 3, block, inner), bf16),
            pltpu.VMEM((chips, 3, block, inner), bf16),
            pltpu.VMEM((chips, 3, block, inner), bf16),
            pltpu.VMEM((chips, 3, block, inner), bf16),
            pltpu.VMEM((chips, 3, block, inner), bf16),
            pltpu.VMEM((2, max(slots - rounds, 1), rows, width), bf16),
            pltpu.SMEM((rounds,), jnp.float32),
            pltpu.SMEM((slots,), jnp.int32),
            pltpu.SMEM((slots,), jnp.float32),
            dma((rounds, n + 2 * (high - 1))),
            dma((rounds, 2, n)),
            dma((rounds,)),
            dma((rounds,)),
            dma((rounds, high)),
            dma((rounds, high)),
            dma((rounds, high)),
            dma((rounds, high)),
            dma((rounds,)),
            dma((rounds,)),
            dma((rounds, 3 + 4 * (chips - 1))),
            dma((rounds, groups)),
            dma((n,)),
            dma((n,)),
            dma((groups,)),
            dma((groups,)),
            dma((chips,)),
            dma((chips,)),
            dma((chips, 3)),
            dma((chips, 3)),
            dma((chips, 3)),
            dma((chips, 3)),
            dma((2,)),
            dma((2,)),
        ],
        compiler_params=pltpu.CompilerParams(
            collective_id=ident, has_side_effects=True, vmem_limit_bytes=60 * 1024 * 1024
        ),
    )(steps, times, tile_map, table, x, cot, gain, w_value, w_gate, w_out)


def emit_kernel(ig_ref, gg_ref, dv_ref, dg_ref, do_ref, a_ref, b_ref, c_ref, d_ref, e_ref):
    a_ref[...] = ig_ref[...]
    b_ref[...] = dv_ref[...]
    c_ref[...] = dg_ref[...]
    d_ref[...] = do_ref[...]
    e_ref[...] = gg_ref[0, :]


def emit(ig, gg, dv, dg, do):
    vmem = pl.BlockSpec(memory_space=pltpu.VMEM)
    outs = [jax.ShapeDtypeStruct(a.shape, a.dtype) for a in (ig, dv, dg, do)]
    outs.append(jax.ShapeDtypeStruct((gg.shape[1],), gg.dtype))
    return pl.pallas_call(
        emit_kernel, in_specs=[vmem] * 5, out_specs=[vmem] * 5, out_shape=outs,
    )(ig, gg, dv, dg, do)


def per_device(latents, cotangent, trunc_steps, timesteps, tile_map, gain, w_value, w_gate, w_out):
    slots = latents.shape[0]
    n, groups = lax.axis_size("tensor"), lax.axis_size("dp")
    table = jnp.asarray(noise_table())
    args = (trunc_steps, timesteps, tile_map, table, latents, cotangent, gain, w_value, w_gate, w_out)
    results = block_backward(n, groups, slots, 0, *args)
    return tuple(emit(*results))


def solution(mesh):
    in_specs = (
        P("dp", "tensor", None),
        P("dp", "tensor", None),
        P(),
        P(),
        P(),
        P(),
        P(None, "tensor"),
        P(None, "tensor"),
        P(None, "tensor"),
    )
    out_specs = (
        P("dp", "tensor", None),
        P("dp", "tensor"),
        P("dp", "tensor"),
        P("dp", "tensor"),
        P(),
    )
    return jax.shard_map(
        per_device, mesh=mesh, in_specs=in_specs, out_specs=out_specs, check_vma=False
    )
```

```python
import functools

import jax
import jax.numpy as jnp
import numpy as np
from jax import lax
from jax.experimental import pallas as pl
from jax.experimental.pallas import tpu as pltpu
from jax.sharding import PartitionSpec as P

eps = 1e-05
early_round = 3


def noise_table():
    betas = np.linspace(0.00085**0.5, 0.012**0.5, 1000) ** 2
    abar = np.exp(np.cumsum(np.log1p(-betas)))
    return np.sqrt(1.0 - abar).astype(np.float32)


def pick(values, index):
    found = values[0]
    for k in range(1, len(values)):
        found = jnp.where(index == k, values[k], found)
    return found


def share(lives, rounds, early):
    over = [jnp.maximum(live - rounds, 0) for live in lives]
    near = [
        jnp.minimum(over[q], jnp.maximum(rounds - lives[q ^ 1], 0)) for q in range(len(lives))
    ]
    spare = [over[q] - near[q] for q in range(len(lives))]
    used = [jnp.minimum(live, rounds) + near[q ^ 1] for q, live in enumerate(lives)]
    begin = [jnp.maximum(u, early) for u in used]
    free = [rounds - b for b in begin]
    spare_at, free_at = [jnp.int32(0)], [jnp.int32(0)]
    for q in range(len(lives)):
        spare_at.append(spare_at[q] + spare[q])
        free_at.append(free_at[q] + free[q])
    return near, used, begin, spare_at, free_at


def block_kernel(n, groups, rounds, ahead, early, steps_ref, times_ref, map_ref, table_ref, x_ref, cot_ref,
                 gain_ref, wv_ref, wg_ref, wo_ref, ig_ref, gg_ref, dv_ref, dg_ref, do_ref,
                 full, part_a, part_b, in_a, in_b, sum_a, sum_b, last_a, last_b, held,
                 acc_v, acc_g, acc_o, placed, gain_one, gain_two,
                 dw_part, dw_pair, dw_sum, dw_down, dw_up, pool_near, pool_far, scale_ref, source_ref,
                 keep_ref, from_ref, near_ref, far_ref, item_ref,
                 ag_send, ag_recv, sa_send, sa_recv, sb_send, sb_recv, ta_send, ta_recv,
                 tb_send, tb_recv, out_send, out_recv, gain_send, gain_recv, far_send, far_recv,
                 pair_send, pair_recv, down_send, down_recv, up_send, up_recv,
                 pool_send, pool_recv):
    slots, rows, width = x_ref.shape
    half = rows // 2
    extra = slots - rounds
    me = lax.axis_index("tensor")
    high = n // 2
    my_high, my_low = me // 2, me % 2
    pair = my_high * 2 + (1 - my_low)
    line_high = [(my_high + k) % high for k in range(1, high)]
    line = [h * 2 + my_low for h in line_high]
    peers = [(me + k) % n for k in range(1, n)]
    first = (((0,), (0,)), ((), ()))
    last = (((1,), (1,)), ((), ()))
    group = lax.axis_index("dp")
    chips = groups // 2
    chip, core = group // 2, group % 2
    twin = chip * 2 + (1 - core)
    block = dw_part.shape[2]
    mate = group + 2 - 4 * (chip % 2)
    base = group // 4 * 4
    lives = [jnp.clip(steps_ref[base + q] - 29, 1, slots) for q in range(4)]
    near, used, first_free, spare_at, free_at = share(lives, rounds, early)
    seat = group % 4
    own_live = pick(lives, seat)
    own_used = pick(used, seat)
    own_begin = pick(first_free, seat)
    own_free_at = pick(free_at[:4], seat)

    def cross(src, dst, send_sem, recv_sem, peer):
        return pltpu.make_async_remote_copy(
            src_ref=src, dst_ref=dst, send_sem=send_sem, recv_sem=recv_sem,
            device_id={"dp": peer}, device_id_type=pl.DeviceIdType.MESH,
        )

    def send(src, dst, send_sem, recv_sem, peer):
        return pltpu.make_async_remote_copy(
            src_ref=src, dst_ref=dst, send_sem=send_sem, recv_sem=recv_sem,
            device_id={"tensor": peer}, device_id_type=pl.DeviceIdType.MESH,
        )

    def out_copy(t, owner, index, peer):
        spot = placed.at[owner * rounds + t]
        return cross(spot, spot, out_send.at[t, index], out_recv.at[t, owner], peer)

    def own_outs(t, act):
        @pl.when(chip + 1 < chips)
        def _():
            act(out_copy(t, group, 0, group + 2))

        @pl.when(chip >= 1)
        def _():
            act(out_copy(t, group, 1, group - 2))

        act(out_copy(t, group, 2, twin))

    def relay_outs(t, d, act, arrive):
        base = 3 + 4 * (d - 1)

        @pl.when(chip >= d)
        def _():
            owner = group - 2 * d
            if arrive:
                out_copy(t, owner, base, twin).wait_recv()

            @pl.when(chip + 1 < chips)
            def _():
                act(out_copy(t, owner, base, group + 2))

            act(out_copy(t, owner, base + 1, twin))

        @pl.when(chip + d < chips)
        def _():
            owner = group + 2 * d
            if arrive:
                out_copy(t, owner, base + 2, twin).wait_recv()

            @pl.when(chip >= 1)
            def _():
                act(out_copy(t, owner, base + 2, group - 2))

            act(out_copy(t, owner, base + 3, twin))

    def begin(copy):
        copy.start()

    def done(copy):
        copy.wait_send()

    def own_copies(t):
        found = []
        for peer in [pair] + line:
            for kind in (0, 1):
                found.append(send(
                    full.at[t, kind, me], full.at[t, kind, me],
                    ag_send.at[t, len(found)], ag_recv.at[t, kind, me], peer,
                ))
        return found

    def passed_copies(t):
        found = []
        base = 2 * high
        for peer in line:
            found.append(send(
                full.at[t, 0, pair], full.at[t, 0, pair],
                ag_send.at[t, base + len(found)], ag_recv.at[t, 0, pair], peer,
            ))
        for owner in line:
            found.append(send(
                full.at[t, 1, owner], full.at[t, 1, owner],
                ag_send.at[t, base + len(found)], ag_recv.at[t, 1, owner], pair,
            ))
        return found

    def arrived(t, kind, owner):
        send(full.at[t, kind, owner], full.at[t, kind, owner], ag_send.at[t, 0],
             ag_recv.at[t, kind, owner], pair).wait_recv()

    def one_a(t):
        return [send(part_a.at[t, 1 - my_low], in_a.at[t], sa_send.at[t], sa_recv.at[t], pair)]

    def one_b(t):
        return [
            send(part_b.at[t, h], in_b.at[t, k], sb_send.at[t, k], sb_recv.at[t, k], p)
            for k, (h, p) in enumerate(zip(line_high, line, strict=True))
        ]

    def two_a(t):
        return [
            send(sum_a.at[t, k], last_a.at[t, k], ta_send.at[t, k], ta_recv.at[t, k], p)
            for k, p in enumerate(line)
        ]

    def two_b(t):
        return [send(sum_b.at[t], last_b.at[t], tb_send.at[t], tb_recv.at[t], pair)]

    def start_own(t):
        for copy in own_copies(t):
            copy.start()

    def pass_on(t):
        for owner in [pair] + line:
            for kind in (0, 1):
                arrived(t, kind, owner)
        for copy in passed_copies(t):
            copy.start()

    barrier = pltpu.get_barrier_semaphore()
    for peer in peers:
        pl.semaphore_signal(
            barrier, inc=1, device_id={"tensor": peer}, device_id_type=pl.DeviceIdType.MESH
        )
    for k in range(1, groups):
        pl.semaphore_signal(
            barrier, inc=1, device_id={"dp": (group + k) % groups},
            device_id_type=pl.DeviceIdType.MESH,
        )
    for kind, ref in enumerate((x_ref, cot_ref)):
        full[0, kind, me] = ref[0]
    pl.semaphore_wait(barrier, n - 1 + groups - 1)
    locals_ = (x_ref, cot_ref) if extra else ()
    near_copies = [
        cross(ref.at[pl.ds(rounds, extra)], pool_near.at[kind], pool_send.at[kind, 0],
              pool_recv.at[kind, 0], twin)
        for kind, ref in enumerate(locals_)
    ]
    far_pool = [
        cross(ref.at[pl.ds(rounds, extra)], pool_far.at[kind, pl.ds(0, extra)],
              pool_send.at[kind, 1], pool_recv.at[kind, 1], mate)
        for kind, ref in enumerate(locals_)
    ]
    far_passed = [
        cross(pool_far.at[kind, pl.ds(0, extra)], pool_far.at[kind, pl.ds(extra, extra)],
              pool_send.at[kind, 2], pool_recv.at[kind, 2], twin)
        for kind, ref in enumerate(locals_)
    ]
    start_own(0)
    for copy in near_copies + far_pool:
        copy.start()

    def set_scale(t, carry):
        mine = t < own_live
        beside = t < own_used
        order = own_free_at + t - own_begin
        item = base * slots
        away_at = jnp.int32(0)
        for q in range(4):
            inside = jnp.logical_and(order >= spare_at[q], order < spare_at[q + 1])
            k = near[q] + order - spare_at[q]
            item = jnp.where(inside, (base + q) * slots + rounds + k, item)
            away_at = jnp.where(inside, jnp.where(core == q % 2, 0, extra) + k, away_at)
        item = jnp.where(beside, twin * slots + rounds + t - own_live, item)
        item = jnp.where(mine, group * slots + t, item)
        item = jnp.clip(item, 0, groups * slots - 1)
        distant = jnp.logical_and(t >= own_begin, order < spare_at[4])
        alive = jnp.logical_or(beside, distant)
        scale_ref[t] = jnp.where(alive, table_ref[times_ref[item]], 0.0)
        from_ref[t] = jnp.where(mine, 0, jnp.where(beside, 1, 2))
        near_ref[t] = jnp.clip(t - own_live, 0, max(extra - 1, 0))
        far_ref[t] = jnp.clip(away_at, 0, max(2 * extra - 1, 0))
        return carry

    lax.fori_loop(0, rounds, set_scale, 0)
    for copy in near_copies:
        copy.wait()

    def fill(t, carry):
        for kind, ref in enumerate((x_ref, cot_ref)):
            tile = ref[t]
            if extra:
                tile = jnp.where(from_ref[t] == 0, tile, pool_near[kind, near_ref[t]])
            full[t, kind, me] = tile
        return carry

    def fill_late(t, carry):
        for kind, ref in enumerate((x_ref, cot_ref)):
            tile = jnp.where(from_ref[t] == 0, ref[t], pool_near[kind, near_ref[t]])
            full[t, kind, me] = jnp.where(from_ref[t] == 2, pool_far[kind, far_ref[t]], tile)
        return carry

    lax.fori_loop(1, early if extra else rounds, fill, 0)
    for t in range(1, min(ahead, rounds)):
        start_own(t)

    def invert(i, found):
        spot = map_ref[i] - group * slots
        return tuple(jnp.where(spot == s, i, item) for s, item in enumerate(found))

    items = lax.fori_loop(0, groups * slots, invert, tuple(jnp.int32(0) for _ in range(slots)))
    for s, item in enumerate(items):
        item_ref[s] = item

    def locate(s, carry):
        item = item_ref[s]
        owner = item // slots
        index = item % slots
        root = owner // 4 * 4
        place_in = owner - root
        there = [jnp.clip(steps_ref[root + q] - 29, 1, slots) for q in range(4)]
        near, used, first_free, spare_at, free_at = share(there, rounds, early)
        other = owner + 1 - 2 * (owner % 2)
        own_near = pick(near, place_in)
        order = pick(spare_at[:4], place_in) + index - rounds - own_near
        spot = jnp.int32(0)
        for q in range(4):
            inside = jnp.logical_and(order >= free_at[q], order < free_at[q + 1])
            spot = jnp.where(
                inside, (root + q) * rounds + first_free[q] + order - free_at[q], spot
            )
        beside = other * rounds + pick([there[q ^ 1] for q in range(4)], place_in) + index - rounds
        spot = jnp.where(index < rounds + own_near, beside, spot)
        spot = jnp.where(index < rounds, owner * rounds + index, spot)
        source_ref[s] = jnp.clip(spot, 0, groups * rounds - 1)
        keep_ref[s] = jnp.where(index < pick(there, place_in), 1.0, 0.0)
        return carry

    lax.fori_loop(0, slots, locate, 0)

    acc_v[...] = jnp.zeros_like(acc_v)
    acc_g[...] = jnp.zeros_like(acc_g)
    acc_o[...] = jnp.zeros_like(acc_o)
    gg_ref[...] = jnp.zeros_like(gg_ref)
    gain = gain_ref[...].reshape(1, width)
    pass_on(0)

    def combine(t):
        for copy in one_a(t):
            copy.wait_recv()
        sums = []
        for h in range(high):
            mine = pick([part_a[t, l, h] for l in range(2)], my_low)
            sums.append(mine.astype(jnp.float32) + in_a[t, h].astype(jnp.float32))
        for k, h in enumerate(line_high):
            sum_a[t, k] = pick(sums, h).astype(jnp.bfloat16)
        for copy in two_a(t):
            copy.start()
        held[t, 0] = pick(sums, my_high)
        for copy in one_b(t):
            copy.wait_recv()
        sums = []
        for l in range(2):
            both = pick([part_b[t, h, l] for h in range(high)], my_high).astype(jnp.float32)
            for k in range(high - 1):
                both += in_b[t, k, l].astype(jnp.float32)
            sums.append(both)
        sum_b[t] = pick(sums, 1 - my_low).astype(jnp.bfloat16)
        for copy in two_b(t):
            copy.start()
        held[t, 1] = pick(sums, my_low)

    def finish(t):
        top = held[t, 0]
        low = held[t, 1]
        for k, copy in enumerate(two_a(t)):
            copy.wait_recv()
            top += last_a[t, k].astype(jnp.float32)
        for copy in two_b(t):
            copy.wait_recv()
        low += last_b[t].astype(jnp.float32)
        d_normed = jnp.concatenate([top, low], axis=0)
        x = full[t, 0, me].astype(jnp.float32)
        centred = x - jnp.mean(x, axis=-1, keepdims=True)
        inv_std = lax.rsqrt(jnp.mean(centred * centred, axis=-1, keepdims=True) + eps)
        x_hat = centred * inv_std
        grad = (full[t, 1, me].astype(jnp.float32) * scale_ref[t]).astype(jnp.bfloat16)
        d_hat = d_normed * gain
        placed[group * rounds + t] = (grad.astype(jnp.float32) + inv_std * (
            d_hat
            - jnp.mean(d_hat, axis=-1, keepdims=True)
            - x_hat * jnp.mean(d_hat * x_hat, axis=-1, keepdims=True)
        )).astype(jnp.bfloat16)
        own_outs(t, begin)
        gg_ref[...] += jnp.sum(d_normed * x_hat, axis=0, keepdims=True)

    def after(t):
        @pl.when(t >= 1)
        def _():
            combine(t - 1)

        @pl.when(t >= 2)
        def _():
            finish(t - 2)

        for d in range(1, chips):
            @pl.when(t >= 2 + d)
            def _():
                relay_outs(t - 2 - d, d, begin, True)

    def relay_left(t):
        for d in range(1, chips):
            if 0 <= t - 2 - d < rounds:
                relay_outs(t - 2 - d, d, begin, True)

    def one_tile(t, carry):
        if extra:
            @pl.when(t == 1)
            def _():
                for copy in far_passed:
                    copy.wait_recv()
                lax.fori_loop(early, rounds, fill_late, 0)

        @pl.when(t + ahead < rounds)
        def _():
            start_own(t + ahead)

        @pl.when(t + 1 < rounds)
        def _():
            pass_on(t + 1)

        far = [h * 2 + (1 - my_low) for h in line_high]
        for owner in far:
            for kind in (0, 1):
                arrived(t, kind, owner)
        x = full[t, 0].reshape(n * rows, width).astype(jnp.float32)
        centred = x - jnp.mean(x, axis=-1, keepdims=True)
        inv_std = lax.rsqrt(jnp.mean(centred * centred, axis=-1, keepdims=True) + eps)
        normed = (centred * inv_std * gain).astype(jnp.bfloat16)
        cot = full[t, 1].reshape(n * rows, width).astype(jnp.float32)
        grad = (cot * scale_ref[t]).astype(jnp.bfloat16)
        values = jnp.dot(normed, wv_ref[...], preferred_element_type=jnp.float32)
        gate = jnp.dot(normed, wg_ref[...], preferred_element_type=jnp.float32)
        d_hidden = jnp.dot(grad, wo_ref[...], preferred_element_type=jnp.float32)
        cdf = 0.5 * (1.0 + lax.erf(gate * 0.7071067811865476))
        density = jnp.exp(-0.5 * gate * gate) * 0.3989422804014327
        gelu = gate * cdf
        hidden = (values * gelu).astype(jnp.bfloat16)
        d_value = (d_hidden * gelu).astype(jnp.bfloat16)
        d_gate = (d_hidden * values * (cdf + gate * density)).astype(jnp.bfloat16)
        d_normed = lax.dot_general(d_value, wv_ref[...], last, preferred_element_type=jnp.float32)
        d_normed += lax.dot_general(d_gate, wg_ref[...], last, preferred_element_type=jnp.float32)
        d_normed = d_normed.astype(jnp.bfloat16).reshape(n, rows, width)
        for h in range(high):
            for l in range(2):
                part_a[t, l, h] = d_normed[h * 2 + l, :half]
                part_b[t, h, l] = d_normed[h * 2 + l, half:]
        for copy in one_a(t) + one_b(t):
            copy.start()
        acc_v[...] += lax.dot_general(normed, d_value, first, preferred_element_type=jnp.float32)
        acc_g[...] += lax.dot_general(normed, d_gate, first, preferred_element_type=jnp.float32)
        acc_o[...] += lax.dot_general(grad, hidden, first, preferred_element_type=jnp.float32)
        if extra:
            @pl.when(t == 0)
            def _():
                for copy in far_pool:
                    copy.wait_recv()
                for copy in far_passed:
                    copy.start()

        after(t)
        return carry

    lax.fori_loop(0, rounds, one_tile, 0)
    pair_copies = [
        cross(dw_part.at[c * 2 + 1 - core], dw_pair.at[c], pair_send.at[c], pair_recv.at[c], twin)
        for c in range(chips)
    ]
    ready = []
    for j in range(chips - 1):
        for c in (j, chips - 1 - j):
            if c not in ready:
                ready.append(c)
                for d in (2 * c, 2 * c + 1):
                    rows_of = slice(d * block, (d + 1) * block)
                    for k, acc in enumerate((acc_v, acc_g, acc_o)):
                        dw_part[d, k] = acc[rows_of, :].astype(jnp.bfloat16)
                pair_copies[c].start()
    combine(rounds - 1)
    if rounds >= 2:
        finish(rounds - 2)
    relay_left(rounds)

    def down_copy(c, k):
        return cross(dw_sum.at[c, k], dw_down.at[c, k], down_send.at[c, k], down_recv.at[c, k],
                     group - 2)

    def up_copy(c, k):
        return cross(dw_sum.at[c, k], dw_up.at[c, k], up_send.at[c, k], up_recv.at[c, k], group + 2)

    def move(j, k):
        @pl.when(chip > j)
        def _():
            @pl.when(chip + 1 < chips)
            def _():
                down_copy(j, k).wait_recv()
                both = dw_sum[j, k].astype(jnp.float32) + dw_down[j, k].astype(jnp.float32)
                dw_sum[j, k] = both.astype(jnp.bfloat16)

            down_copy(j, k).start()

        c = chips - 1 - j

        @pl.when(chip < c)
        def _():
            @pl.when(chip >= 1)
            def _():
                up_copy(c, k).wait_recv()
                both = dw_sum[c, k].astype(jnp.float32) + dw_up[c, k].astype(jnp.float32)
                dw_sum[c, k] = both.astype(jnp.bfloat16)

            up_copy(c, k).start()

    gain_copies = [
        send(gg_ref, gain_one.at[me], gain_send.at[k], gain_recv.at[me], peer)
        for k, peer in enumerate(peers)
    ]
    left = list(range(rounds + 2, rounds + 1 + chips))
    for j in range(chips - 1):
        for c in (j, chips - 1 - j):
            if c in ready:
                ready.remove(c)
                pair_copies[c].wait()
                both = dw_part[c * 2 + core].astype(jnp.float32) + dw_pair[c].astype(jnp.float32)
                dw_sum[c] = both.astype(jnp.bfloat16)
        for k in range(3):
            move(j, k)
            if j == 0 and k == 0:
                finish(rounds - 1)
                relay_left(rounds + 1)
                gain_one[me] = gg_ref[...]
                for copy in gain_copies:
                    copy.start()
            elif j >= 1 and k != 1 and left:
                relay_left(left.pop(0))
    for t in left:
        relay_left(t)
    for peer in peers:
        send(gg_ref, gain_one.at[peer], gain_send.at[0], gain_recv.at[peer], peer).wait_recv()
    for copy in gain_copies:
        copy.wait_send()
    gain_sum = gain_one[0]
    for k in range(1, n):
        gain_sum += gain_one[k]
    gain_two[group] = gain_sum
    far_copies = [
        cross(gain_two.at[group], gain_two.at[group], far_send.at[k], far_recv.at[group],
              (group + k) % groups)
        for k in range(1, groups)
    ]
    for copy in far_copies:
        copy.start()

    def settle(t, carry):
        for c in range(chips):
            out_copy(t, c * 2 + 1 - core, 0, twin).wait_recv()
        for copy in (own_copies(t) + passed_copies(t) + one_a(t) + one_b(t) + two_a(t) + two_b(t)):
            copy.wait_send()
        own_outs(t, done)
        for d in range(1, chips):
            relay_outs(t, d, done, False)
        return carry

    lax.fori_loop(0, rounds, settle, 0)
    for copy in far_pool + far_passed:
        copy.wait_send()

    def place(t, carry):
        ig_ref[t] = (placed[source_ref[t]].astype(jnp.float32) * keep_ref[t]).astype(jnp.bfloat16)
        return carry

    lax.fori_loop(0, slots, place, 0)
    for k in range(1, groups):
        peer = (group + k) % groups
        cross(gain_two.at[peer], gain_two.at[peer], far_send.at[k], far_recv.at[peer],
              peer).wait_recv()
    for copy in far_copies:
        copy.wait_send()
    gain_total = gain_two[0]
    for k in range(1, groups):
        gain_total += gain_two[k]
    gg_ref[...] = gain_total
    outs = (dv_ref, dg_ref, do_ref)
    for c in range(chips):
        @pl.when(chip == c)
        def _():
            for k, ref in enumerate(outs):
                total = dw_sum[c, k].astype(jnp.float32)
                if c + 1 < chips:
                    down_copy(c, k).wait_recv()
                    total += dw_down[c, k].astype(jnp.float32)
                if c >= 1:
                    up_copy(c, k).wait_recv()
                    total += dw_up[c, k].astype(jnp.float32)
                ref[...] = total

    for j in range(chips - 1):
        for k in range(3):
            @pl.when(chip > j)
            def _():
                down_copy(j, k).wait_send()

            @pl.when(chip < chips - 1 - j)
            def _():
                up_copy(chips - 1 - j, k).wait_send()


def block_backward(n, groups, rounds, ident, steps, times, tile_map, table, x, cot, gain,
                   w_value, w_gate, w_out):
    slots, rows, width = x.shape
    inner = w_value.shape[1]
    chips = groups // 2
    high = n // 2
    half = rows // 2
    others = max(high - 1, 1)
    block = width // groups
    vmem = pl.BlockSpec(memory_space=pltpu.VMEM)
    smem = pl.BlockSpec(memory_space=pltpu.SMEM)
    grads = jax.ShapeDtypeStruct((block, inner), jnp.float32)
    dma = pltpu.SemaphoreType.DMA
    bf16 = jnp.bfloat16
    return pl.pallas_call(
        functools.partial(block_kernel, n, groups, rounds, 2, min(early_round, rounds)),
        in_specs=[smem] * 4 + [vmem] * 6,
        out_specs=[vmem] * 5,
        out_shape=[
            jax.ShapeDtypeStruct((slots, rows, width), bf16),
            jax.ShapeDtypeStruct((1, width), jnp.float32),
            grads,
            grads,
            grads,
        ],
        scratch_shapes=[
            pltpu.VMEM((rounds, 2, n, rows, width), bf16),
            pltpu.VMEM((rounds, 2, high, half, width), bf16),
            pltpu.VMEM((rounds, high, 2, half, width), bf16),
            pltpu.VMEM((rounds, high, half, width), bf16),
            pltpu.VMEM((rounds, others, 2, half, width), bf16),
            pltpu.VMEM((rounds, others, half, width), bf16),
            pltpu.VMEM((rounds, half, width), bf16),
            pltpu.VMEM((rounds, others, half, width), bf16),
            pltpu.VMEM((rounds, half, width), bf16),
            pltpu.VMEM((rounds, 2, half, width), jnp.float32),
        ]
        + [pltpu.VMEM((width, inner), jnp.float32)] * 3
        + [
            pltpu.VMEM((groups * rounds, rows, width), bf16),
            pltpu.VMEM((n, 1, width), jnp.float32),
            pltpu.VMEM((groups, 1, width), jnp.float32),
            pltpu.VMEM((groups, 3, block, inner), bf16),
            pltpu.VMEM((chips, 3, block, inner), bf16),
            pltpu.VMEM((chips, 3, block, inner), bf16),
            pltpu.VMEM((chips, 3, block, inner), bf16),
            pltpu.VMEM((chips, 3, block, inner), bf16),
            pltpu.VMEM((2, max(slots - rounds, 1), rows, width), bf16),
            pltpu.VMEM((2, max(2 * (slots - rounds), 1), rows, width), bf16),
            pltpu.SMEM((rounds,), jnp.float32),
            pltpu.SMEM((slots,), jnp.int32),
            pltpu.SMEM((slots,), jnp.float32),
            pltpu.SMEM((rounds,), jnp.int32),
            pltpu.SMEM((rounds,), jnp.int32),
            pltpu.SMEM((rounds,), jnp.int32),
            pltpu.SMEM((slots,), jnp.int32),
            dma((rounds, n + 2 * (high - 1))),
            dma((rounds, 2, n)),
            dma((rounds,)),
            dma((rounds,)),
            dma((rounds, high)),
            dma((rounds, high)),
            dma((rounds, high)),
            dma((rounds, high)),
            dma((rounds,)),
            dma((rounds,)),
            dma((rounds, 3 + 4 * (chips - 1))),
            dma((rounds, groups)),
            dma((n,)),
            dma((n,)),
            dma((groups,)),
            dma((groups,)),
            dma((chips,)),
            dma((chips,)),
            dma((chips, 3)),
            dma((chips, 3)),
            dma((chips, 3)),
            dma((chips, 3)),
            dma((2, 3)),
            dma((2, 3)),
        ],
        compiler_params=pltpu.CompilerParams(
            collective_id=ident, has_side_effects=True, vmem_limit_bytes=60 * 1024 * 1024
        ),
    )(steps, times, tile_map, table, x, cot, gain, w_value, w_gate, w_out)


def emit_kernel(ig_ref, gg_ref, dv_ref, dg_ref, do_ref, a_ref, b_ref, c_ref, d_ref, e_ref):
    a_ref[...] = ig_ref[...]
    b_ref[...] = dv_ref[...]
    c_ref[...] = dg_ref[...]
    d_ref[...] = do_ref[...]
    e_ref[...] = gg_ref[0, :]


def emit(ig, gg, dv, dg, do):
    vmem = pl.BlockSpec(memory_space=pltpu.VMEM)
    outs = [jax.ShapeDtypeStruct(a.shape, a.dtype) for a in (ig, dv, dg, do)]
    outs.append(jax.ShapeDtypeStruct((gg.shape[1],), gg.dtype))
    return pl.pallas_call(
        emit_kernel, in_specs=[vmem] * 5, out_specs=[vmem] * 5, out_shape=outs,
    )(ig, gg, dv, dg, do)


def choose_kernel(plans, groups, slots, steps_ref, choice_ref):
    choice = jnp.int32(0)
    blocked = jnp.int32(1)
    for rounds in plans[:-1]:
        lacking = jnp.int32(0)
        for base in range(0, groups, 4):
            lives = [jnp.clip(steps_ref[base + q] - 29, 1, slots) for q in range(4)]
            _, _, _, spare_at, free_at = share(lives, rounds, min(early_round, rounds))
            lacking = jnp.maximum(lacking, spare_at[4] - free_at[4])
        blocked = jnp.where(lacking > 0, blocked, 0)
        choice = choice + blocked
    choice_ref[0] = choice


def choose(plans, groups, slots, steps):
    smem = pl.BlockSpec(memory_space=pltpu.SMEM)
    return pl.pallas_call(
        functools.partial(choose_kernel, plans, groups, slots), in_specs=[smem], out_specs=smem,
        out_shape=jax.ShapeDtypeStruct((1,), jnp.int32),
    )(steps)[0]


def per_device(latents, cotangent, trunc_steps, timesteps, tile_map, gain, w_value, w_gate, w_out):
    slots = latents.shape[0]
    n, groups = lax.axis_size("tensor"), lax.axis_size("dp")
    table = jnp.asarray(noise_table())
    args = (trunc_steps, timesteps, tile_map, table, latents, cotangent, gain, w_value, w_gate, w_out)
    plans = [r for r in (6, 7, 8) if r < slots] + [slots]
    choice = choose(plans, groups, slots, trunc_steps)
    results = lax.switch(
        choice, [functools.partial(block_backward, n, groups, r, k) for k, r in enumerate(plans)],
        *args,
    )
    return tuple(emit(*results))


def solution(mesh):
    in_specs = (
        P("dp", "tensor", None),
        P("dp", "tensor", None),
        P(),
        P(),
        P(),
        P(),
        P(None, "tensor"),
        P(None, "tensor"),
        P(None, "tensor"),
    )
    out_specs = (
        P("dp", "tensor", None),
        P("dp", "tensor"),
        P("dp", "tensor"),
        P("dp", "tensor"),
        P(),
    )
    return jax.shard_map(
        per_device, mesh=mesh, in_specs=in_specs, out_specs=out_specs, check_vma=False
    )
```

```python
import functools

import jax
import jax.numpy as jnp
import numpy as np
from jax import lax
from jax.experimental import pallas as pl
from jax.experimental.pallas import tpu as pltpu
from jax.sharding import PartitionSpec as P

eps = 1e-05
early_round = 3


def noise_table():
    betas = np.linspace(0.00085**0.5, 0.012**0.5, 1000) ** 2
    abar = np.exp(np.cumsum(np.log1p(-betas)))
    return np.sqrt(1.0 - abar).astype(np.float32)


def pick(values, index):
    found = values[0]
    for k in range(1, len(values)):
        found = jnp.where(index == k, values[k], found)
    return found


def share(lives, rounds, early):
    over = [jnp.maximum(live - rounds, 0) for live in lives]
    near = [
        jnp.minimum(over[q], jnp.maximum(rounds - lives[q ^ 1], 0)) for q in range(len(lives))
    ]
    spare = [over[q] - near[q] for q in range(len(lives))]
    used = [jnp.minimum(live, rounds) + near[q ^ 1] for q, live in enumerate(lives)]
    begin = [jnp.maximum(u, early) for u in used]
    free = [rounds - b for b in begin]
    spare_at, free_at = [jnp.int32(0)], [jnp.int32(0)]
    for q in range(len(lives)):
        spare_at.append(spare_at[q] + spare[q])
        free_at.append(free_at[q] + free[q])
    return near, used, begin, spare_at, free_at


def block_kernel(n, groups, rounds, ahead, early, lag, late, steps_ref, times_ref, map_ref, table_ref, x_ref, cot_ref,
                 gain_ref, wv_ref, wg_ref, wo_ref, ig_ref, gg_ref, dv_ref, dg_ref, do_ref,
                 full, part_a, part_b, in_a, in_b, sum_a, sum_b, last_a, last_b, held,
                 acc_v, acc_g, acc_o, placed, gain_one, gain_two,
                 dw_part, dw_pair, dw_sum, dw_down, dw_up, pool_near, pool_far, scale_ref, source_ref,
                 keep_ref, from_ref, near_ref, far_ref, item_ref,
                 ag_send, ag_recv, sa_send, sa_recv, sb_send, sb_recv, ta_send, ta_recv,
                 tb_send, tb_recv, out_send, out_recv, gain_send, gain_recv, far_send, far_recv,
                 pair_send, pair_recv, down_send, down_recv, up_send, up_recv,
                 pool_send, pool_recv):
    slots, rows, width = x_ref.shape
    half = rows // 2
    extra = slots - rounds
    me = lax.axis_index("tensor")
    high = n // 2
    my_high, my_low = me // 2, me % 2
    pair = my_high * 2 + (1 - my_low)
    line_high = [(my_high + k) % high for k in range(1, high)]
    line = [h * 2 + my_low for h in line_high]
    peers = [(me + k) % n for k in range(1, n)]
    first = (((0,), (0,)), ((), ()))
    last = (((1,), (1,)), ((), ()))
    group = lax.axis_index("dp")
    chips = groups // 2
    chip, core = group // 2, group % 2
    twin = chip * 2 + (1 - core)
    block = dw_part.shape[2]
    mate = group + 2 - 4 * (chip % 2)
    base = group // 4 * 4
    lives = [jnp.clip(steps_ref[base + q] - 29, 1, slots) for q in range(4)]
    near, used, first_free, spare_at, free_at = share(lives, rounds, early)
    seat = group % 4
    own_live = pick(lives, seat)
    own_used = pick(used, seat)
    own_begin = pick(first_free, seat)
    own_free_at = pick(free_at[:4], seat)

    def cross(src, dst, send_sem, recv_sem, peer):
        return pltpu.make_async_remote_copy(
            src_ref=src, dst_ref=dst, send_sem=send_sem, recv_sem=recv_sem,
            device_id={"dp": peer}, device_id_type=pl.DeviceIdType.MESH,
        )

    def send(src, dst, send_sem, recv_sem, peer):
        return pltpu.make_async_remote_copy(
            src_ref=src, dst_ref=dst, send_sem=send_sem, recv_sem=recv_sem,
            device_id={"tensor": peer}, device_id_type=pl.DeviceIdType.MESH,
        )

    def out_copy(t, owner, index, peer):
        spot = placed.at[owner * rounds + t]
        return cross(spot, spot, out_send.at[t, index], out_recv.at[t, owner], peer)

    def own_outs(t, act):
        @pl.when(chip + 1 < chips)
        def _():
            act(out_copy(t, group, 0, group + 2))

        @pl.when(chip >= 1)
        def _():
            act(out_copy(t, group, 1, group - 2))

        act(out_copy(t, group, 2, twin))

    def relay_outs(t, d, act, arrive):
        base = 3 + 4 * (d - 1)

        @pl.when(chip >= d)
        def _():
            owner = group - 2 * d
            if arrive:
                out_copy(t, owner, base, twin).wait_recv()

            @pl.when(chip + 1 < chips)
            def _():
                act(out_copy(t, owner, base, group + 2))

            act(out_copy(t, owner, base + 1, twin))

        @pl.when(chip + d < chips)
        def _():
            owner = group + 2 * d
            if arrive:
                out_copy(t, owner, base + 2, twin).wait_recv()

            @pl.when(chip >= 1)
            def _():
                act(out_copy(t, owner, base + 2, group - 2))

            act(out_copy(t, owner, base + 3, twin))

    def begin(copy):
        copy.start()

    def done(copy):
        copy.wait_send()

    def own_copies(t):
        found = []
        for peer in [pair] + line:
            for kind in (0, 1):
                found.append(send(
                    full.at[t, kind, me], full.at[t, kind, me],
                    ag_send.at[t, len(found)], ag_recv.at[t, kind, me], peer,
                ))
        return found

    def passed_copies(t):
        found = []
        base = 2 * high
        for peer in line:
            found.append(send(
                full.at[t, 0, pair], full.at[t, 0, pair],
                ag_send.at[t, base + len(found)], ag_recv.at[t, 0, pair], peer,
            ))
        for owner in line:
            found.append(send(
                full.at[t, 1, owner], full.at[t, 1, owner],
                ag_send.at[t, base + len(found)], ag_recv.at[t, 1, owner], pair,
            ))
        return found

    def arrived(t, kind, owner):
        send(full.at[t, kind, owner], full.at[t, kind, owner], ag_send.at[t, 0],
             ag_recv.at[t, kind, owner], pair).wait_recv()

    def one_a(t):
        return [send(part_a.at[t, 1 - my_low], in_a.at[t], sa_send.at[t], sa_recv.at[t], pair)]

    def one_b(t):
        return [
            send(part_b.at[t, h], in_b.at[t, k], sb_send.at[t, k], sb_recv.at[t, k], p)
            for k, (h, p) in enumerate(zip(line_high, line, strict=True))
        ]

    def two_a(t):
        return [
            send(sum_a.at[t, k], last_a.at[t, k], ta_send.at[t, k], ta_recv.at[t, k], p)
            for k, p in enumerate(line)
        ]

    def two_b(t):
        return [send(sum_b.at[t], last_b.at[t], tb_send.at[t], tb_recv.at[t], pair)]

    def start_own(t):
        for copy in own_copies(t):
            copy.start()

    def pass_on(t):
        for owner in [pair] + line:
            for kind in (0, 1):
                arrived(t, kind, owner)
        for copy in passed_copies(t):
            copy.start()

    barrier = pltpu.get_barrier_semaphore()
    for peer in peers:
        pl.semaphore_signal(
            barrier, inc=1, device_id={"tensor": peer}, device_id_type=pl.DeviceIdType.MESH
        )
    for k in range(1, groups):
        pl.semaphore_signal(
            barrier, inc=1, device_id={"dp": (group + k) % groups},
            device_id_type=pl.DeviceIdType.MESH,
        )
    for kind, ref in enumerate((x_ref, cot_ref)):
        full[0, kind, me] = ref[0]
    pl.semaphore_wait(barrier, n - 1 + groups - 1)
    locals_ = (x_ref, cot_ref) if extra else ()
    near_copies = [
        cross(ref.at[pl.ds(rounds, extra)], pool_near.at[kind], pool_send.at[kind, 0],
              pool_recv.at[kind, 0], twin)
        for kind, ref in enumerate(locals_)
    ]
    far_pool = [
        cross(ref.at[pl.ds(rounds, extra)], pool_far.at[kind, pl.ds(0, extra)],
              pool_send.at[kind, 1], pool_recv.at[kind, 1], mate)
        for kind, ref in enumerate(locals_)
    ]
    far_passed = [
        cross(pool_far.at[kind, pl.ds(0, extra)], pool_far.at[kind, pl.ds(extra, extra)],
              pool_send.at[kind, 2], pool_recv.at[kind, 2], twin)
        for kind, ref in enumerate(locals_)
    ]
    start_own(0)
    for copy in near_copies + far_pool:
        copy.start()

    def set_scale(t, carry):
        mine = t < own_live
        beside = t < own_used
        order = own_free_at + t - own_begin
        item = base * slots
        away_at = jnp.int32(0)
        for q in range(4):
            inside = jnp.logical_and(order >= spare_at[q], order < spare_at[q + 1])
            k = near[q] + order - spare_at[q]
            item = jnp.where(inside, (base + q) * slots + rounds + k, item)
            away_at = jnp.where(inside, jnp.where(core == q % 2, 0, extra) + k, away_at)
        item = jnp.where(beside, twin * slots + rounds + t - own_live, item)
        item = jnp.where(mine, group * slots + t, item)
        item = jnp.clip(item, 0, groups * slots - 1)
        distant = jnp.logical_and(t >= own_begin, order < spare_at[4])
        alive = jnp.logical_or(beside, distant)
        scale_ref[t] = jnp.where(alive, table_ref[times_ref[item]], 0.0)
        from_ref[t] = jnp.where(mine, 0, jnp.where(beside, 1, 2))
        near_ref[t] = jnp.clip(t - own_live, 0, max(extra - 1, 0))
        far_ref[t] = jnp.clip(away_at, 0, max(2 * extra - 1, 0))
        return carry

    lax.fori_loop(0, rounds, set_scale, 0)
    for copy in near_copies:
        copy.wait()

    def fill(t, carry):
        for kind, ref in enumerate((x_ref, cot_ref)):
            tile = ref[t]
            if extra:
                tile = jnp.where(from_ref[t] == 0, tile, pool_near[kind, near_ref[t]])
            full[t, kind, me] = tile
        return carry

    def fill_late(t, carry):
        for kind, ref in enumerate((x_ref, cot_ref)):
            tile = jnp.where(from_ref[t] == 0, ref[t], pool_near[kind, near_ref[t]])
            full[t, kind, me] = jnp.where(from_ref[t] == 2, pool_far[kind, far_ref[t]], tile)
        return carry

    lax.fori_loop(1, early if extra else rounds, fill, 0)
    started = min(ahead + 1, early if extra else rounds)
    for t in range(1, started):
        start_own(t)

    def invert(i, found):
        spot = map_ref[i] - group * slots
        return tuple(jnp.where(spot == s, i, item) for s, item in enumerate(found))

    items = lax.fori_loop(0, groups * slots, invert, tuple(jnp.int32(0) for _ in range(slots)))
    for s, item in enumerate(items):
        item_ref[s] = item

    def locate(s, carry):
        item = item_ref[s]
        owner = item // slots
        index = item % slots
        root = owner // 4 * 4
        place_in = owner - root
        there = [jnp.clip(steps_ref[root + q] - 29, 1, slots) for q in range(4)]
        near, used, first_free, spare_at, free_at = share(there, rounds, early)
        other = owner + 1 - 2 * (owner % 2)
        own_near = pick(near, place_in)
        order = pick(spare_at[:4], place_in) + index - rounds - own_near
        spot = jnp.int32(0)
        for q in range(4):
            inside = jnp.logical_and(order >= free_at[q], order < free_at[q + 1])
            spot = jnp.where(
                inside, (root + q) * rounds + first_free[q] + order - free_at[q], spot
            )
        beside = other * rounds + pick([there[q ^ 1] for q in range(4)], place_in) + index - rounds
        spot = jnp.where(index < rounds + own_near, beside, spot)
        spot = jnp.where(index < rounds, owner * rounds + index, spot)
        source_ref[s] = jnp.clip(spot, 0, groups * rounds - 1)
        keep_ref[s] = jnp.where(index < pick(there, place_in), 1.0, 0.0)
        return carry

    lax.fori_loop(0, slots, locate, 0)

    acc_v[...] = jnp.zeros_like(acc_v)
    acc_g[...] = jnp.zeros_like(acc_g)
    acc_o[...] = jnp.zeros_like(acc_o)
    gg_ref[...] = jnp.zeros_like(gg_ref)
    gain = gain_ref[...].reshape(1, width)
    pass_on(0)

    def combine(t):
        for copy in one_a(t):
            copy.wait_recv()
        sums = []
        for h in range(high):
            mine = pick([part_a[t, l, h] for l in range(2)], my_low)
            sums.append(mine.astype(jnp.float32) + in_a[t, h].astype(jnp.float32))
        for k, h in enumerate(line_high):
            sum_a[t, k] = pick(sums, h).astype(jnp.bfloat16)
        for copy in two_a(t):
            copy.start()
        held[t, 0] = pick(sums, my_high)
        for copy in one_b(t):
            copy.wait_recv()
        sums = []
        for l in range(2):
            both = pick([part_b[t, h, l] for h in range(high)], my_high).astype(jnp.float32)
            for k in range(high - 1):
                both += in_b[t, k, l].astype(jnp.float32)
            sums.append(both)
        sum_b[t] = pick(sums, 1 - my_low).astype(jnp.bfloat16)
        for copy in two_b(t):
            copy.start()
        held[t, 1] = pick(sums, my_low)

    def finish(t):
        top = held[t, 0]
        low = held[t, 1]
        for k, copy in enumerate(two_a(t)):
            copy.wait_recv()
            top += last_a[t, k].astype(jnp.float32)
        for copy in two_b(t):
            copy.wait_recv()
        low += last_b[t].astype(jnp.float32)
        d_normed = jnp.concatenate([top, low], axis=0)
        x = full[t, 0, me].astype(jnp.float32)
        centred = x - jnp.mean(x, axis=-1, keepdims=True)
        inv_std = lax.rsqrt(jnp.mean(centred * centred, axis=-1, keepdims=True) + eps)
        x_hat = centred * inv_std
        grad = (full[t, 1, me].astype(jnp.float32) * scale_ref[t]).astype(jnp.bfloat16)
        d_hat = d_normed * gain
        placed[group * rounds + t] = (grad.astype(jnp.float32) + inv_std * (
            d_hat
            - jnp.mean(d_hat, axis=-1, keepdims=True)
            - x_hat * jnp.mean(d_hat * x_hat, axis=-1, keepdims=True)
        )).astype(jnp.bfloat16)
        own_outs(t, begin)
        gg_ref[...] += jnp.sum(d_normed * x_hat, axis=0, keepdims=True)

    def after(t):
        @pl.when(t >= lag)
        def _():
            combine(t - lag)

        @pl.when(t >= late)
        def _():
            finish(t - late)

        for d in range(1, chips):
            @pl.when(t >= late + d)
            def _():
                relay_outs(t - late - d, d, begin, True)

    def relay_left(t):
        for d in range(1, chips):
            if 0 <= t - late - d < rounds:
                relay_outs(t - late - d, d, begin, True)

    def one_tile(t, carry):
        @pl.when(t == 1)
        def _():
            if extra:
                for copy in far_passed:
                    copy.wait_recv()
                lax.fori_loop(early, rounds, fill_late, 0)
            for later in range(started, min(ahead + 2, rounds)):
                start_own(later)

        @pl.when(t >= 2)
        def _():
            @pl.when(t + ahead < rounds)
            def _():
                start_own(t + ahead)

        @pl.when(t + 1 < rounds)
        def _():
            pass_on(t + 1)

        far = [h * 2 + (1 - my_low) for h in line_high]
        for owner in far:
            for kind in (0, 1):
                arrived(t, kind, owner)
        x = full[t, 0].reshape(n * rows, width).astype(jnp.float32)
        centred = x - jnp.mean(x, axis=-1, keepdims=True)
        inv_std = lax.rsqrt(jnp.mean(centred * centred, axis=-1, keepdims=True) + eps)
        normed = (centred * inv_std * gain).astype(jnp.bfloat16)
        cot = full[t, 1].reshape(n * rows, width).astype(jnp.float32)
        grad = (cot * scale_ref[t]).astype(jnp.bfloat16)
        values = jnp.dot(normed, wv_ref[...], preferred_element_type=jnp.float32)
        gate = jnp.dot(normed, wg_ref[...], preferred_element_type=jnp.float32)
        d_hidden = jnp.dot(grad, wo_ref[...], preferred_element_type=jnp.float32)
        cdf = 0.5 * (1.0 + lax.erf(gate * 0.7071067811865476))
        density = jnp.exp(-0.5 * gate * gate) * 0.3989422804014327
        gelu = gate * cdf
        hidden = (values * gelu).astype(jnp.bfloat16)
        d_value = (d_hidden * gelu).astype(jnp.bfloat16)
        d_gate = (d_hidden * values * (cdf + gate * density)).astype(jnp.bfloat16)
        d_normed = lax.dot_general(d_value, wv_ref[...], last, preferred_element_type=jnp.float32)
        d_normed += lax.dot_general(d_gate, wg_ref[...], last, preferred_element_type=jnp.float32)
        d_normed = d_normed.astype(jnp.bfloat16).reshape(n, rows, width)
        for h in range(high):
            for l in range(2):
                part_a[t, l, h] = d_normed[h * 2 + l, :half]
                part_b[t, h, l] = d_normed[h * 2 + l, half:]
        for copy in one_a(t) + one_b(t):
            copy.start()
        acc_v[...] += lax.dot_general(normed, d_value, first, preferred_element_type=jnp.float32)
        acc_g[...] += lax.dot_general(normed, d_gate, first, preferred_element_type=jnp.float32)
        acc_o[...] += lax.dot_general(grad, hidden, first, preferred_element_type=jnp.float32)
        if extra:
            @pl.when(t == 0)
            def _():
                for copy in far_pool:
                    copy.wait_recv()
                for copy in far_passed:
                    copy.start()

        after(t)
        return carry

    lax.fori_loop(0, rounds, one_tile, 0)
    pair_copies = [
        cross(dw_part.at[c * 2 + 1 - core], dw_pair.at[c], pair_send.at[c], pair_recv.at[c], twin)
        for c in range(chips)
    ]
    ready = []
    for j in range(chips - 1):
        for c in (j, chips - 1 - j):
            if c not in ready:
                ready.append(c)
                for d in (2 * c, 2 * c + 1):
                    rows_of = slice(d * block, (d + 1) * block)
                    for k, acc in enumerate((acc_v, acc_g, acc_o)):
                        dw_part[d, k] = acc[rows_of, :].astype(jnp.bfloat16)
                pair_copies[c].start()
    for t in range(rounds, rounds + late - 1):
        if t - lag < rounds:
            combine(t - lag)
        if t >= late:
            finish(t - late)
        relay_left(t)

    def down_copy(c, k):
        return cross(dw_sum.at[c, k], dw_down.at[c, k], down_send.at[c, k], down_recv.at[c, k],
                     group - 2)

    def up_copy(c, k):
        return cross(dw_sum.at[c, k], dw_up.at[c, k], up_send.at[c, k], up_recv.at[c, k], group + 2)

    def move(j, k):
        c = chips - 1 - j

        @pl.when(chip > j)
        def _():
            @pl.when(chip + 1 < chips)
            def _():
                down_copy(j, k).wait_recv()
                both = dw_sum[j, k].astype(jnp.float32) + dw_down[j, k].astype(jnp.float32)
                dw_sum[j, k] = both.astype(jnp.bfloat16)
                down_copy(j, k).start()

        @pl.when(chip < c)
        def _():
            @pl.when(chip >= 1)
            def _():
                up_copy(c, k).wait_recv()
                both = dw_sum[c, k].astype(jnp.float32) + dw_up[c, k].astype(jnp.float32)
                dw_sum[c, k] = both.astype(jnp.bfloat16)
                up_copy(c, k).start()

    gain_copies = [
        send(gg_ref, gain_one.at[me], gain_send.at[k], gain_recv.at[me], peer)
        for k, peer in enumerate(peers)
    ]
    for c in ready:
        pair_copies[c].wait()
        both = dw_part[c * 2 + core].astype(jnp.float32) + dw_pair[c].astype(jnp.float32)
        dw_sum[c] = both.astype(jnp.bfloat16)
    finish(rounds - 1)
    parts = [(j, k) for j in range(chips - 1) for k in range(3)]
    for j, k in parts:
        @pl.when(chip == chips - 1)
        def _():
            down_copy(j, k).start()

        @pl.when(chip == 0)
        def _():
            up_copy(chips - 1 - j, k).start()

    relay_left(rounds + late - 1)
    gain_one[me] = gg_ref[...]
    for copy in gain_copies:
        copy.start()
    left = list(range(rounds + late, rounds + late - 1 + chips))
    for index, (j, k) in enumerate(parts):
        if index != 1 and left:
            relay_left(left.pop(0))
        move(j, k)
    for t in left:
        relay_left(t)
    for peer in peers:
        send(gg_ref, gain_one.at[peer], gain_send.at[0], gain_recv.at[peer], peer).wait_recv()
    for copy in gain_copies:
        copy.wait_send()
    gain_sum = gain_one[0]
    for k in range(1, n):
        gain_sum += gain_one[k]
    gain_two[group] = gain_sum
    far_copies = [
        cross(gain_two.at[group], gain_two.at[group], far_send.at[k], far_recv.at[group],
              (group + k) % groups)
        for k in range(1, groups)
    ]
    for copy in far_copies:
        copy.start()

    def settle(t, carry):
        for c in range(chips):
            out_copy(t, c * 2 + 1 - core, 0, twin).wait_recv()
        for copy in (own_copies(t) + passed_copies(t) + one_a(t) + one_b(t) + two_a(t) + two_b(t)):
            copy.wait_send()
        own_outs(t, done)
        for d in range(1, chips):
            relay_outs(t, d, done, False)
        return carry

    lax.fori_loop(0, rounds, settle, 0)
    for copy in far_pool + far_passed:
        copy.wait_send()

    def place(t, carry):
        ig_ref[t] = (placed[source_ref[t]].astype(jnp.float32) * keep_ref[t]).astype(jnp.bfloat16)
        return carry

    lax.fori_loop(0, slots, place, 0)
    for k in range(1, groups):
        peer = (group + k) % groups
        cross(gain_two.at[peer], gain_two.at[peer], far_send.at[k], far_recv.at[peer],
              peer).wait_recv()
    for copy in far_copies:
        copy.wait_send()
    gain_total = gain_two[0]
    for k in range(1, groups):
        gain_total += gain_two[k]
    gg_ref[...] = gain_total
    outs = (dv_ref, dg_ref, do_ref)
    for c in range(chips):
        @pl.when(chip == c)
        def _():
            for k, ref in enumerate(outs):
                total = dw_sum[c, k].astype(jnp.float32)
                if c + 1 < chips:
                    down_copy(c, k).wait_recv()
                    total += dw_down[c, k].astype(jnp.float32)
                if c >= 1:
                    up_copy(c, k).wait_recv()
                    total += dw_up[c, k].astype(jnp.float32)
                ref[...] = total

    for j in range(chips - 1):
        for k in range(3):
            @pl.when(chip > j)
            def _():
                down_copy(j, k).wait_send()

            @pl.when(chip < chips - 1 - j)
            def _():
                up_copy(chips - 1 - j, k).wait_send()


def block_backward(n, groups, rounds, ident, steps, times, tile_map, table, x, cot, gain,
                   w_value, w_gate, w_out):
    slots, rows, width = x.shape
    inner = w_value.shape[1]
    chips = groups // 2
    high = n // 2
    half = rows // 2
    others = max(high - 1, 1)
    block = width // groups
    vmem = pl.BlockSpec(memory_space=pltpu.VMEM)
    smem = pl.BlockSpec(memory_space=pltpu.SMEM)
    grads = jax.ShapeDtypeStruct((block, inner), jnp.float32)
    dma = pltpu.SemaphoreType.DMA
    bf16 = jnp.bfloat16
    return pl.pallas_call(
        functools.partial(block_kernel, n, groups, rounds, 2, min(early_round, rounds), 1, 2),
        in_specs=[smem] * 4 + [vmem] * 6,
        out_specs=[vmem] * 5,
        out_shape=[
            jax.ShapeDtypeStruct((slots, rows, width), bf16),
            jax.ShapeDtypeStruct((1, width), jnp.float32),
            grads,
            grads,
            grads,
        ],
        scratch_shapes=[
            pltpu.VMEM((rounds, 2, n, rows, width), bf16),
            pltpu.VMEM((rounds, 2, high, half, width), bf16),
            pltpu.VMEM((rounds, high, 2, half, width), bf16),
            pltpu.VMEM((rounds, high, half, width), bf16),
            pltpu.VMEM((rounds, others, 2, half, width), bf16),
            pltpu.VMEM((rounds, others, half, width), bf16),
            pltpu.VMEM((rounds, half, width), bf16),
            pltpu.VMEM((rounds, others, half, width), bf16),
            pltpu.VMEM((rounds, half, width), bf16),
            pltpu.VMEM((rounds, 2, half, width), jnp.float32),
        ]
        + [pltpu.VMEM((width, inner), jnp.float32)] * 3
        + [
            pltpu.VMEM((groups * rounds, rows, width), bf16),
            pltpu.VMEM((n, 1, width), jnp.float32),
            pltpu.VMEM((groups, 1, width), jnp.float32),
            pltpu.VMEM((groups, 3, block, inner), bf16),
            pltpu.VMEM((chips, 3, block, inner), bf16),
            pltpu.VMEM((chips, 3, block, inner), bf16),
            pltpu.VMEM((chips, 3, block, inner), bf16),
            pltpu.VMEM((chips, 3, block, inner), bf16),
            pltpu.VMEM((2, max(slots - rounds, 1), rows, width), bf16),
            pltpu.VMEM((2, max(2 * (slots - rounds), 1), rows, width), bf16),
            pltpu.SMEM((rounds,), jnp.float32),
            pltpu.SMEM((slots,), jnp.int32),
            pltpu.SMEM((slots,), jnp.float32),
            pltpu.SMEM((rounds,), jnp.int32),
            pltpu.SMEM((rounds,), jnp.int32),
            pltpu.SMEM((rounds,), jnp.int32),
            pltpu.SMEM((slots,), jnp.int32),
            dma((rounds, n + 2 * (high - 1))),
            dma((rounds, 2, n)),
            dma((rounds,)),
            dma((rounds,)),
            dma((rounds, high)),
            dma((rounds, high)),
            dma((rounds, high)),
            dma((rounds, high)),
            dma((rounds,)),
            dma((rounds,)),
            dma((rounds, 3 + 4 * (chips - 1))),
            dma((rounds, groups)),
            dma((n,)),
            dma((n,)),
            dma((groups,)),
            dma((groups,)),
            dma((chips,)),
            dma((chips,)),
            dma((chips, 3)),
            dma((chips, 3)),
            dma((chips, 3)),
            dma((chips, 3)),
            dma((2, 3)),
            dma((2, 3)),
        ],
        compiler_params=pltpu.CompilerParams(
            collective_id=ident, has_side_effects=True, vmem_limit_bytes=60 * 1024 * 1024
        ),
    )(steps, times, tile_map, table, x, cot, gain, w_value, w_gate, w_out)


def emit_kernel(ig_ref, gg_ref, dv_ref, dg_ref, do_ref, a_ref, b_ref, c_ref, d_ref, e_ref):
    a_ref[...] = ig_ref[...]
    b_ref[...] = dv_ref[...]
    c_ref[...] = dg_ref[...]
    d_ref[...] = do_ref[...]
    e_ref[...] = gg_ref[0, :]


def emit(ig, gg, dv, dg, do):
    vmem = pl.BlockSpec(memory_space=pltpu.VMEM)
    outs = [jax.ShapeDtypeStruct(a.shape, a.dtype) for a in (ig, dv, dg, do)]
    outs.append(jax.ShapeDtypeStruct((gg.shape[1],), gg.dtype))
    return pl.pallas_call(
        emit_kernel, in_specs=[vmem] * 5, out_specs=[vmem] * 5, out_shape=outs,
    )(ig, gg, dv, dg, do)


def choose_kernel(plans, groups, slots, steps_ref, choice_ref):
    choice = jnp.int32(0)
    blocked = jnp.int32(1)
    for rounds in plans[:-1]:
        lacking = jnp.int32(0)
        for base in range(0, groups, 4):
            lives = [jnp.clip(steps_ref[base + q] - 29, 1, slots) for q in range(4)]
            _, _, _, spare_at, free_at = share(lives, rounds, min(early_round, rounds))
            lacking = jnp.maximum(lacking, spare_at[4] - free_at[4])
        blocked = jnp.where(lacking > 0, blocked, 0)
        choice = choice + blocked
    choice_ref[0] = choice


def choose(plans, groups, slots, steps):
    smem = pl.BlockSpec(memory_space=pltpu.SMEM)
    return pl.pallas_call(
        functools.partial(choose_kernel, plans, groups, slots), in_specs=[smem], out_specs=smem,
        out_shape=jax.ShapeDtypeStruct((1,), jnp.int32),
    )(steps)[0]


def per_device(latents, cotangent, trunc_steps, timesteps, tile_map, gain, w_value, w_gate, w_out):
    slots = latents.shape[0]
    n, groups = lax.axis_size("tensor"), lax.axis_size("dp")
    table = jnp.asarray(noise_table())
    args = (trunc_steps, timesteps, tile_map, table, latents, cotangent, gain, w_value, w_gate, w_out)
    plans = [r for r in (6, 7, 8) if r < slots] + [slots]
    choice = choose(plans, groups, slots, trunc_steps)
    results = lax.switch(
        choice, [functools.partial(block_backward, n, groups, r, k) for k, r in enumerate(plans)],
        *args,
    )
    return tuple(emit(*results))


def solution(mesh):
    in_specs = (
        P("dp", "tensor", None),
        P("dp", "tensor", None),
        P(),
        P(),
        P(),
        P(),
        P(None, "tensor"),
        P(None, "tensor"),
        P(None, "tensor"),
    )
    out_specs = (
        P("dp", "tensor", None),
        P("dp", "tensor"),
        P("dp", "tensor"),
        P("dp", "tensor"),
        P(),
    )
    return jax.shard_map(
        per_device, mesh=mesh, in_specs=in_specs, out_specs=out_specs, check_vma=False
    )
```

```python
import functools

import jax
import jax.numpy as jnp
import numpy as np
from jax import lax
from jax.experimental import pallas as pl
from jax.experimental.pallas import tpu as pltpu
from jax.sharding import PartitionSpec as P

eps = 1e-05
early_round = 3


def noise_table():
    betas = np.linspace(0.00085**0.5, 0.012**0.5, 1000) ** 2
    abar = np.exp(np.cumsum(np.log1p(-betas)))
    return np.sqrt(1.0 - abar).astype(np.float32)


def pick(values, index):
    found = values[0]
    for k in range(1, len(values)):
        found = jnp.where(index == k, values[k], found)
    return found


def share(lives, rounds, early):
    over = [jnp.maximum(live - rounds, 0) for live in lives]
    near = [
        jnp.minimum(over[q], jnp.maximum(rounds - lives[q ^ 1], 0)) for q in range(len(lives))
    ]
    spare = [over[q] - near[q] for q in range(len(lives))]
    used = [jnp.minimum(live, rounds) + near[q ^ 1] for q, live in enumerate(lives)]
    begin = [jnp.maximum(u, early) for u in used]
    free = [rounds - b for b in begin]
    spare_at, free_at = [jnp.int32(0)], [jnp.int32(0)]
    for q in range(len(lives)):
        spare_at.append(spare_at[q] + spare[q])
        free_at.append(free_at[q] + free[q])
    return near, used, begin, spare_at, free_at


def block_kernel(n, groups, rounds, ahead, early, lag, late, steps_ref, times_ref, map_ref, table_ref, x_ref, cot_ref,
                 gain_ref, wv_ref, wg_ref, wo_ref, ig_ref, gg_ref, dv_ref, dg_ref, do_ref,
                 full, part_a, part_b, in_a, in_b, sum_a, sum_b, last_a, last_b, held,
                 acc_v, acc_g, acc_o, placed, gain_one, gain_two,
                 dw_part, dw_pair, dw_sum, dw_down, dw_up, pool_near, pool_far, scale_ref, source_ref,
                 keep_ref, from_ref, near_ref, far_ref, item_ref,
                 ag_send, ag_recv, sa_send, sa_recv, sb_send, sb_recv, ta_send, ta_recv,
                 tb_send, tb_recv, out_send, out_recv, gain_send, gain_recv, far_send, far_recv,
                 pair_send, pair_recv, down_send, down_recv, up_send, up_recv,
                 pool_send, pool_recv):
    slots, rows, width = x_ref.shape
    half = rows // 2
    extra = slots - rounds
    me = lax.axis_index("tensor")
    high = n // 2
    my_high, my_low = me // 2, me % 2
    pair = my_high * 2 + (1 - my_low)
    line_high = [(my_high + k) % high for k in range(1, high)]
    line = [h * 2 + my_low for h in line_high]
    peers = [(me + k) % n for k in range(1, n)]
    first = (((0,), (0,)), ((), ()))
    last = (((1,), (1,)), ((), ()))
    group = lax.axis_index("dp")
    chips = groups // 2
    chip, core = group // 2, group % 2
    twin = chip * 2 + (1 - core)
    block = dw_part.shape[2]
    mate = group + 2 - 4 * (chip % 2)
    base = group // 4 * 4
    lives = [jnp.clip(steps_ref[base + q] - 29, 1, slots) for q in range(4)]
    near, used, first_free, spare_at, free_at = share(lives, rounds, early)
    seat = group % 4
    own_live = pick(lives, seat)
    own_used = pick(used, seat)
    own_begin = pick(first_free, seat)
    own_free_at = pick(free_at[:4], seat)

    def cross(src, dst, send_sem, recv_sem, peer):
        return pltpu.make_async_remote_copy(
            src_ref=src, dst_ref=dst, send_sem=send_sem, recv_sem=recv_sem,
            device_id={"dp": peer}, device_id_type=pl.DeviceIdType.MESH,
        )

    def send(src, dst, send_sem, recv_sem, peer):
        return pltpu.make_async_remote_copy(
            src_ref=src, dst_ref=dst, send_sem=send_sem, recv_sem=recv_sem,
            device_id={"tensor": peer}, device_id_type=pl.DeviceIdType.MESH,
        )

    def out_copy(t, owner, index, peer):
        spot = placed.at[owner * rounds + t]
        return cross(spot, spot, out_send.at[t, index], out_recv.at[t, owner], peer)

    def own_outs(t, act):
        @pl.when(chip + 1 < chips)
        def _():
            act(out_copy(t, group, 0, group + 2))

        @pl.when(chip >= 1)
        def _():
            act(out_copy(t, group, 1, group - 2))

        act(out_copy(t, group, 2, twin))

    def relay_outs(t, d, act, arrive):
        base = 3 + 4 * (d - 1)

        @pl.when(chip >= d)
        def _():
            owner = group - 2 * d
            if arrive:
                out_copy(t, owner, base, twin).wait_recv()

            @pl.when(chip + 1 < chips)
            def _():
                act(out_copy(t, owner, base, group + 2))

            act(out_copy(t, owner, base + 1, twin))

        @pl.when(chip + d < chips)
        def _():
            owner = group + 2 * d
            if arrive:
                out_copy(t, owner, base + 2, twin).wait_recv()

            @pl.when(chip >= 1)
            def _():
                act(out_copy(t, owner, base + 2, group - 2))

            act(out_copy(t, owner, base + 3, twin))

    def begin(copy):
        copy.start()

    def done(copy):
        copy.wait_send()

    def own_copies(t):
        found = []
        for peer in [pair] + line:
            for kind in (0, 1):
                found.append(send(
                    full.at[t, kind, me], full.at[t, kind, me],
                    ag_send.at[t, len(found)], ag_recv.at[t, kind, me], peer,
                ))
        return found

    def passed_copies(t):
        found = []
        base = 2 * high
        for peer in line:
            found.append(send(
                full.at[t, 0, pair], full.at[t, 0, pair],
                ag_send.at[t, base + len(found)], ag_recv.at[t, 0, pair], peer,
            ))
        for owner in line:
            found.append(send(
                full.at[t, 1, owner], full.at[t, 1, owner],
                ag_send.at[t, base + len(found)], ag_recv.at[t, 1, owner], pair,
            ))
        return found

    def arrived(t, kind, owner):
        send(full.at[t, kind, owner], full.at[t, kind, owner], ag_send.at[t, 0],
             ag_recv.at[t, kind, owner], pair).wait_recv()

    def one_a(t):
        return [send(part_a.at[t, 1 - my_low], in_a.at[t], sa_send.at[t], sa_recv.at[t], pair)]

    def one_b(t):
        return [
            send(part_b.at[t, h], in_b.at[t, k], sb_send.at[t, k], sb_recv.at[t, k], p)
            for k, (h, p) in enumerate(zip(line_high, line, strict=True))
        ]

    def two_a(t):
        return [
            send(sum_a.at[t, k], last_a.at[t, k], ta_send.at[t, k], ta_recv.at[t, k], p)
            for k, p in enumerate(line)
        ]

    def two_b(t):
        return [send(sum_b.at[t], last_b.at[t], tb_send.at[t], tb_recv.at[t], pair)]

    def start_own(t):
        for copy in own_copies(t):
            copy.start()

    def pass_on(t):
        for owner in [pair] + line:
            for kind in (0, 1):
                arrived(t, kind, owner)
        for copy in passed_copies(t):
            copy.start()

    barrier = pltpu.get_barrier_semaphore()
    for peer in peers:
        pl.semaphore_signal(
            barrier, inc=1, device_id={"tensor": peer}, device_id_type=pl.DeviceIdType.MESH
        )
    for k in range(1, groups):
        pl.semaphore_signal(
            barrier, inc=1, device_id={"dp": (group + k) % groups},
            device_id_type=pl.DeviceIdType.MESH,
        )
    for kind, ref in enumerate((x_ref, cot_ref)):
        full[0, kind, me] = ref[0]
    pl.semaphore_wait(barrier, n - 1 + groups - 1)
    locals_ = (x_ref, cot_ref) if extra else ()
    near_copies = [
        cross(ref.at[pl.ds(rounds, extra)], pool_near.at[kind], pool_send.at[kind, 0],
              pool_recv.at[kind, 0], twin)
        for kind, ref in enumerate(locals_)
    ]
    far_pool = [
        cross(ref.at[pl.ds(rounds, extra)], pool_far.at[kind, pl.ds(0, extra)],
              pool_send.at[kind, 1], pool_recv.at[kind, 1], mate)
        for kind, ref in enumerate(locals_)
    ]
    far_passed = [
        cross(pool_far.at[kind, pl.ds(0, extra)], pool_far.at[kind, pl.ds(extra, extra)],
              pool_send.at[kind, 2], pool_recv.at[kind, 2], twin)
        for kind, ref in enumerate(locals_)
    ]
    start_own(0)
    for copy in near_copies + far_pool:
        copy.start()

    def set_scale(t, carry):
        mine = t < own_live
        beside = t < own_used
        order = own_free_at + t - own_begin
        item = base * slots
        away_at = jnp.int32(0)
        for q in range(4):
            inside = jnp.logical_and(order >= spare_at[q], order < spare_at[q + 1])
            k = near[q] + order - spare_at[q]
            item = jnp.where(inside, (base + q) * slots + rounds + k, item)
            away_at = jnp.where(inside, jnp.where(core == q % 2, 0, extra) + k, away_at)
        item = jnp.where(beside, twin * slots + rounds + t - own_live, item)
        item = jnp.where(mine, group * slots + t, item)
        item = jnp.clip(item, 0, groups * slots - 1)
        distant = jnp.logical_and(t >= own_begin, order < spare_at[4])
        alive = jnp.logical_or(beside, distant)
        scale_ref[t] = jnp.where(alive, table_ref[times_ref[item]], 0.0)
        from_ref[t] = jnp.where(mine, 0, jnp.where(beside, 1, 2))
        near_ref[t] = jnp.clip(t - own_live, 0, max(extra - 1, 0))
        far_ref[t] = jnp.clip(away_at, 0, max(2 * extra - 1, 0))
        return carry

    lax.fori_loop(0, rounds, set_scale, 0)
    for copy in near_copies:
        copy.wait()

    def fill(t, carry):
        for kind, ref in enumerate((x_ref, cot_ref)):
            tile = ref[t]
            if extra:
                tile = jnp.where(from_ref[t] == 0, tile, pool_near[kind, near_ref[t]])
            full[t, kind, me] = tile
        return carry

    def fill_late(t, carry):
        for kind, ref in enumerate((x_ref, cot_ref)):
            tile = jnp.where(from_ref[t] == 0, ref[t], pool_near[kind, near_ref[t]])
            full[t, kind, me] = jnp.where(from_ref[t] == 2, pool_far[kind, far_ref[t]], tile)
        return carry

    lax.fori_loop(1, early if extra else rounds, fill, 0)
    started = min(ahead + 1, early if extra else rounds)
    for t in range(1, started):
        start_own(t)

    def invert(i, found):
        spot = map_ref[i] - group * slots
        return tuple(jnp.where(spot == s, i, item) for s, item in enumerate(found))

    items = lax.fori_loop(0, groups * slots, invert, tuple(jnp.int32(0) for _ in range(slots)))
    for s, item in enumerate(items):
        item_ref[s] = item

    def locate(s, carry):
        item = item_ref[s]
        owner = item // slots
        index = item % slots
        root = owner // 4 * 4
        place_in = owner - root
        there = [jnp.clip(steps_ref[root + q] - 29, 1, slots) for q in range(4)]
        near, used, first_free, spare_at, free_at = share(there, rounds, early)
        other = owner + 1 - 2 * (owner % 2)
        own_near = pick(near, place_in)
        order = pick(spare_at[:4], place_in) + index - rounds - own_near
        spot = jnp.int32(0)
        for q in range(4):
            inside = jnp.logical_and(order >= free_at[q], order < free_at[q + 1])
            spot = jnp.where(
                inside, (root + q) * rounds + first_free[q] + order - free_at[q], spot
            )
        beside = other * rounds + pick([there[q ^ 1] for q in range(4)], place_in) + index - rounds
        spot = jnp.where(index < rounds + own_near, beside, spot)
        spot = jnp.where(index < rounds, owner * rounds + index, spot)
        source_ref[s] = jnp.clip(spot, 0, groups * rounds - 1)
        keep_ref[s] = jnp.where(index < pick(there, place_in), 1.0, 0.0)
        return carry

    lax.fori_loop(0, slots, locate, 0)

    inner = acc_v.shape[1]

    def clear(d, carry):
        for acc in (acc_v, acc_g, acc_o):
            acc[pl.ds(pl.multiple_of(d * block, 8), block), :] = jnp.zeros(
                (block, inner), jnp.float32
            )
        return carry

    lax.fori_loop(0, groups, clear, 0)
    gg_ref[...] = jnp.zeros_like(gg_ref)
    gain = gain_ref[...].reshape(1, width)
    pass_on(0)

    def combine(t):
        for copy in one_a(t):
            copy.wait_recv()
        sums = []
        for h in range(high):
            mine = pick([part_a[t, l, h] for l in range(2)], my_low)
            sums.append(mine.astype(jnp.float32) + in_a[t, h].astype(jnp.float32))
        for k, h in enumerate(line_high):
            sum_a[t, k] = pick(sums, h).astype(jnp.bfloat16)
        for copy in two_a(t):
            copy.start()
        held[t, 0] = pick(sums, my_high)
        for copy in one_b(t):
            copy.wait_recv()
        sums = []
        for l in range(2):
            both = pick([part_b[t, h, l] for h in range(high)], my_high).astype(jnp.float32)
            for k in range(high - 1):
                both += in_b[t, k, l].astype(jnp.float32)
            sums.append(both)
        sum_b[t] = pick(sums, 1 - my_low).astype(jnp.bfloat16)
        for copy in two_b(t):
            copy.start()
        held[t, 1] = pick(sums, my_low)

    def finish(t):
        top = held[t, 0]
        low = held[t, 1]
        for k, copy in enumerate(two_a(t)):
            copy.wait_recv()
            top += last_a[t, k].astype(jnp.float32)
        for copy in two_b(t):
            copy.wait_recv()
        low += last_b[t].astype(jnp.float32)
        d_normed = jnp.concatenate([top, low], axis=0)
        x = full[t, 0, me].astype(jnp.float32)
        centred = x - jnp.mean(x, axis=-1, keepdims=True)
        inv_std = lax.rsqrt(jnp.mean(centred * centred, axis=-1, keepdims=True) + eps)
        x_hat = centred * inv_std
        grad = (full[t, 1, me].astype(jnp.float32) * scale_ref[t]).astype(jnp.bfloat16)
        d_hat = d_normed * gain
        placed[group * rounds + t] = (grad.astype(jnp.float32) + inv_std * (
            d_hat
            - jnp.mean(d_hat, axis=-1, keepdims=True)
            - x_hat * jnp.mean(d_hat * x_hat, axis=-1, keepdims=True)
        )).astype(jnp.bfloat16)
        own_outs(t, begin)
        gg_ref[...] += jnp.sum(d_normed * x_hat, axis=0, keepdims=True)

    def after(t):
        @pl.when(t >= lag)
        def _():
            combine(t - lag)

        @pl.when(t >= late)
        def _():
            finish(t - late)

        for d in range(1, chips):
            @pl.when(t >= late + d)
            def _():
                relay_outs(t - late - d, d, begin, True)

    def relay_left(t):
        for d in range(1, chips):
            if 0 <= t - late - d < rounds:
                relay_outs(t - late - d, d, begin, True)

    def one_tile(t, carry):
        @pl.when(t == 1)
        def _():
            if extra:
                for copy in far_passed:
                    copy.wait_recv()
                lax.fori_loop(early, rounds, fill_late, 0)
            for later in range(started, min(ahead + 2, rounds)):
                start_own(later)

        @pl.when(t >= 2)
        def _():
            @pl.when(t + ahead < rounds)
            def _():
                start_own(t + ahead)

        @pl.when(t + 1 < rounds)
        def _():
            pass_on(t + 1)

        far = [h * 2 + (1 - my_low) for h in line_high]
        for owner in far:
            for kind in (0, 1):
                arrived(t, kind, owner)
        x = full[t, 0].reshape(n * rows, width).astype(jnp.float32)
        centred = x - jnp.mean(x, axis=-1, keepdims=True)
        inv_std = lax.rsqrt(jnp.mean(centred * centred, axis=-1, keepdims=True) + eps)
        normed = (centred * inv_std * gain).astype(jnp.bfloat16)
        cot = full[t, 1].reshape(n * rows, width).astype(jnp.float32)
        grad = (cot * scale_ref[t]).astype(jnp.bfloat16)
        values = jnp.dot(normed, wv_ref[...], preferred_element_type=jnp.float32)
        gate = jnp.dot(normed, wg_ref[...], preferred_element_type=jnp.float32)
        d_hidden = jnp.dot(grad, wo_ref[...], preferred_element_type=jnp.float32)
        cdf = 0.5 * (1.0 + lax.erf(gate * 0.7071067811865476))
        density = jnp.exp(-0.5 * gate * gate) * 0.3989422804014327
        gelu = gate * cdf
        hidden = (values * gelu).astype(jnp.bfloat16)
        d_value = (d_hidden * gelu).astype(jnp.bfloat16)
        d_gate = (d_hidden * values * (cdf + gate * density)).astype(jnp.bfloat16)
        d_normed = lax.dot_general(d_value, wv_ref[...], last, preferred_element_type=jnp.float32)
        d_normed += lax.dot_general(d_gate, wg_ref[...], last, preferred_element_type=jnp.float32)
        d_normed = d_normed.astype(jnp.bfloat16).reshape(n, rows, width)
        for h in range(high):
            for l in range(2):
                part_a[t, l, h] = d_normed[h * 2 + l, :half]
                part_b[t, h, l] = d_normed[h * 2 + l, half:]
        for copy in one_a(t) + one_b(t):
            copy.start()
        acc_v[...] += lax.dot_general(normed, d_value, first, preferred_element_type=jnp.float32)
        acc_g[...] += lax.dot_general(normed, d_gate, first, preferred_element_type=jnp.float32)
        acc_o[...] += lax.dot_general(grad, hidden, first, preferred_element_type=jnp.float32)
        if extra:
            @pl.when(t == 0)
            def _():
                for copy in far_pool:
                    copy.wait_recv()
                for copy in far_passed:
                    copy.start()

        after(t)
        return carry

    lax.fori_loop(0, rounds, one_tile, 0)
    pair_copies = [
        cross(dw_part.at[c * 2 + 1 - core], dw_pair.at[c], pair_send.at[c], pair_recv.at[c], twin)
        for c in range(chips)
    ]

    def narrow(d, carry):
        for k, acc in enumerate((acc_v, acc_g, acc_o)):
            part = acc[pl.ds(pl.multiple_of(d * block, 8), block), :]
            dw_part[d, k] = part.astype(jnp.bfloat16)
        return carry

    ready = []
    for j in range(chips - 1):
        for c in (j, chips - 1 - j):
            if c not in ready:
                ready.append(c)
                lax.fori_loop(2 * c, 2 * c + 2, narrow, 0)
                pair_copies[c].start()
    for t in range(rounds, rounds + late - 1):
        if t - lag < rounds:
            combine(t - lag)
        if t >= late:
            finish(t - late)
        relay_left(t)

    def down_copy(c, k):
        return cross(dw_sum.at[c, k], dw_down.at[c, k], down_send.at[c, k], down_recv.at[c, k],
                     group - 2)

    def up_copy(c, k):
        return cross(dw_sum.at[c, k], dw_up.at[c, k], up_send.at[c, k], up_recv.at[c, k], group + 2)

    def move(j, k):
        c = chips - 1 - j

        @pl.when(chip > j)
        def _():
            @pl.when(chip + 1 < chips)
            def _():
                down_copy(j, k).wait_recv()
                both = dw_sum[j, k].astype(jnp.float32) + dw_down[j, k].astype(jnp.float32)
                dw_sum[j, k] = both.astype(jnp.bfloat16)
                down_copy(j, k).start()

        @pl.when(chip < c)
        def _():
            @pl.when(chip >= 1)
            def _():
                up_copy(c, k).wait_recv()
                both = dw_sum[c, k].astype(jnp.float32) + dw_up[c, k].astype(jnp.float32)
                dw_sum[c, k] = both.astype(jnp.bfloat16)
                up_copy(c, k).start()

    gain_copies = [
        send(gg_ref, gain_one.at[me], gain_send.at[k], gain_recv.at[me], peer)
        for k, peer in enumerate(peers)
    ]
    for c in ready:
        pair_copies[c].wait()

        def add_pair(k, carry):
            both = dw_part[c * 2 + core, k].astype(jnp.float32) + dw_pair[c, k].astype(jnp.float32)
            dw_sum[c, k] = both.astype(jnp.bfloat16)
            return carry

        lax.fori_loop(0, 3, add_pair, 0)

    parts = [(j, k) for j in range(chips - 1) for k in range(3)]

    def kick(some):
        @pl.when(chip == chips - 1)
        def _():
            for j, k in some:
                down_copy(j, k).start()

        @pl.when(chip == 0)
        def _():
            for j, k in some:
                up_copy(chips - 1 - j, k).start()

    kick(parts[:1])
    finish(rounds - 1)
    kick(parts[1:])
    relay_left(rounds + late - 1)
    gain_one[me] = gg_ref[...]
    for copy in gain_copies:
        copy.start()
    far_copies = [
        cross(gain_two.at[group], gain_two.at[group], far_send.at[k], far_recv.at[group],
              (group + k) % groups)
        for k in range(1, groups)
    ]

    def share_gain():
        for peer in peers:
            send(gg_ref, gain_one.at[peer], gain_send.at[0], gain_recv.at[peer], peer).wait_recv()
        for copy in gain_copies:
            copy.wait_send()
        gain_sum = gain_one[0]
        for k in range(1, n):
            gain_sum += gain_one[k]
        gain_two[group] = gain_sum
        for copy in far_copies:
            copy.start()

    moved = {}
    left = list(range(rounds + late, rounds + late - 1 + chips))
    for index, (j, k) in enumerate(parts):
        if index != 1 and left:
            relay_left(left.pop(0))
        if index == 1:
            share_gain()
        if j < 1 or len(left) > 0:
            move(j, k)
        elif k == 0 or not moved.get(j):
            moved[j] = True

            def move_rest(part, carry):
                move(j, part)
                return carry

            lax.fori_loop(k, 3, move_rest, 0)
    for t in left:
        relay_left(t)
    def settle(t, carry):
        for c in range(chips):
            out_copy(t, c * 2 + 1 - core, 0, twin).wait_recv()
        for copy in (own_copies(t) + passed_copies(t) + one_a(t) + one_b(t) + two_a(t) + two_b(t)):
            copy.wait_send()
        own_outs(t, done)
        for d in range(1, chips):
            relay_outs(t, d, done, False)
        return carry

    lax.fori_loop(0, rounds, settle, 0)
    for copy in far_pool + far_passed:
        copy.wait_send()

    def place(t, carry):
        ig_ref[t] = (placed[source_ref[t]].astype(jnp.float32) * keep_ref[t]).astype(jnp.bfloat16)
        return carry

    lax.fori_loop(0, slots, place, 0)
    for k in range(1, groups):
        peer = (group + k) % groups
        cross(gain_two.at[peer], gain_two.at[peer], far_send.at[k], far_recv.at[peer],
              peer).wait_recv()
    for copy in far_copies:
        copy.wait_send()
    gain_total = gain_two[0]
    for k in range(1, groups):
        gain_total += gain_two[k]
    gg_ref[...] = gain_total
    outs = (dv_ref, dg_ref, do_ref)
    for k, ref in enumerate(outs):
        ref[...] = dw_sum[chip, k].astype(jnp.float32)

    @pl.when(chip + 1 < chips)
    def _():
        for k in range(3):
            down_copy(chip, k).wait_recv()
        for k, ref in enumerate(outs):
            ref[...] += dw_down[chip, k].astype(jnp.float32)

    @pl.when(chip >= 1)
    def _():
        for k in range(3):
            up_copy(chip, k).wait_recv()
        for k, ref in enumerate(outs):
            ref[...] += dw_up[chip, k].astype(jnp.float32)

    for j in range(chips - 1):
        for k in range(3):
            @pl.when(chip > j)
            def _():
                down_copy(j, k).wait_send()

            @pl.when(chip < chips - 1 - j)
            def _():
                up_copy(chips - 1 - j, k).wait_send()


def block_backward(n, groups, rounds, ident, steps, times, tile_map, table, x, cot, gain,
                   w_value, w_gate, w_out):
    slots, rows, width = x.shape
    inner = w_value.shape[1]
    chips = groups // 2
    high = n // 2
    half = rows // 2
    others = max(high - 1, 1)
    block = width // groups
    vmem = pl.BlockSpec(memory_space=pltpu.VMEM)
    smem = pl.BlockSpec(memory_space=pltpu.SMEM)
    grads = jax.ShapeDtypeStruct((block, inner), jnp.float32)
    dma = pltpu.SemaphoreType.DMA
    bf16 = jnp.bfloat16
    return pl.pallas_call(
        functools.partial(block_kernel, n, groups, rounds, 2, min(early_round, rounds), 1, 2),
        in_specs=[smem] * 4 + [vmem] * 6,
        out_specs=[vmem] * 5,
        out_shape=[
            jax.ShapeDtypeStruct((slots, rows, width), bf16),
            jax.ShapeDtypeStruct((1, width), jnp.float32),
            grads,
            grads,
            grads,
        ],
        scratch_shapes=[
            pltpu.VMEM((rounds, 2, n, rows, width), bf16),
            pltpu.VMEM((rounds, 2, high, half, width), bf16),
            pltpu.VMEM((rounds, high, 2, half, width), bf16),
            pltpu.VMEM((rounds, high, half, width), bf16),
            pltpu.VMEM((rounds, others, 2, half, width), bf16),
            pltpu.VMEM((rounds, others, half, width), bf16),
            pltpu.VMEM((rounds, half, width), bf16),
            pltpu.VMEM((rounds, others, half, width), bf16),
            pltpu.VMEM((rounds, half, width), bf16),
            pltpu.VMEM((rounds, 2, half, width), jnp.float32),
        ]
        + [pltpu.VMEM((width, inner), jnp.float32)] * 3
        + [
            pltpu.VMEM((groups * rounds, rows, width), bf16),
            pltpu.VMEM((n, 1, width), jnp.float32),
            pltpu.VMEM((groups, 1, width), jnp.float32),
            pltpu.VMEM((groups, 3, block, inner), bf16),
            pltpu.VMEM((chips, 3, block, inner), bf16),
            pltpu.VMEM((chips, 3, block, inner), bf16),
            pltpu.VMEM((chips, 3, block, inner), bf16),
            pltpu.VMEM((chips, 3, block, inner), bf16),
            pltpu.VMEM((2, max(slots - rounds, 1), rows, width), bf16),
            pltpu.VMEM((2, max(2 * (slots - rounds), 1), rows, width), bf16),
            pltpu.SMEM((rounds,), jnp.float32),
            pltpu.SMEM((slots,), jnp.int32),
            pltpu.SMEM((slots,), jnp.float32),
            pltpu.SMEM((rounds,), jnp.int32),
            pltpu.SMEM((rounds,), jnp.int32),
            pltpu.SMEM((rounds,), jnp.int32),
            pltpu.SMEM((slots,), jnp.int32),
            dma((rounds, n + 2 * (high - 1))),
            dma((rounds, 2, n)),
            dma((rounds,)),
            dma((rounds,)),
            dma((rounds, high)),
            dma((rounds, high)),
            dma((rounds, high)),
            dma((rounds, high)),
            dma((rounds,)),
            dma((rounds,)),
            dma((rounds, 3 + 4 * (chips - 1))),
            dma((rounds, groups)),
            dma((n,)),
            dma((n,)),
            dma((groups,)),
            dma((groups,)),
            dma((chips,)),
            dma((chips,)),
            dma((chips, 3)),
            dma((chips, 3)),
            dma((chips, 3)),
            dma((chips, 3)),
            dma((2, 3)),
            dma((2, 3)),
        ],
        compiler_params=pltpu.CompilerParams(
            collective_id=ident, has_side_effects=True, vmem_limit_bytes=60 * 1024 * 1024
        ),
    )(steps, times, tile_map, table, x, cot, gain, w_value, w_gate, w_out)


def emit_kernel(ig_ref, gg_ref, dv_ref, dg_ref, do_ref, a_ref, b_ref, c_ref, d_ref, e_ref):
    a_ref[...] = ig_ref[...]
    b_ref[...] = dv_ref[...]
    c_ref[...] = dg_ref[...]
    d_ref[...] = do_ref[...]
    e_ref[...] = gg_ref[0, :]


def emit(ig, gg, dv, dg, do):
    vmem = pl.BlockSpec(memory_space=pltpu.VMEM)
    outs = [jax.ShapeDtypeStruct(a.shape, a.dtype) for a in (ig, dv, dg, do)]
    outs.append(jax.ShapeDtypeStruct((gg.shape[1],), gg.dtype))
    return pl.pallas_call(
        emit_kernel, in_specs=[vmem] * 5, out_specs=[vmem] * 5, out_shape=outs,
    )(ig, gg, dv, dg, do)


def choose_kernel(plans, groups, slots, steps_ref, choice_ref):
    choice = jnp.int32(0)
    blocked = jnp.int32(1)
    for rounds in plans[:-1]:
        lacking = jnp.int32(0)
        for base in range(0, groups, 4):
            lives = [jnp.clip(steps_ref[base + q] - 29, 1, slots) for q in range(4)]
            _, _, _, spare_at, free_at = share(lives, rounds, min(early_round, rounds))
            lacking = jnp.maximum(lacking, spare_at[4] - free_at[4])
        blocked = jnp.where(lacking > 0, blocked, 0)
        choice = choice + blocked
    choice_ref[0] = choice


def choose(plans, groups, slots, steps):
    smem = pl.BlockSpec(memory_space=pltpu.SMEM)
    return pl.pallas_call(
        functools.partial(choose_kernel, plans, groups, slots), in_specs=[smem], out_specs=smem,
        out_shape=jax.ShapeDtypeStruct((1,), jnp.int32),
    )(steps)[0]


def per_device(latents, cotangent, trunc_steps, timesteps, tile_map, gain, w_value, w_gate, w_out):
    slots = latents.shape[0]
    n, groups = lax.axis_size("tensor"), lax.axis_size("dp")
    table = jnp.asarray(noise_table())
    args = (trunc_steps, timesteps, tile_map, table, latents, cotangent, gain, w_value, w_gate, w_out)
    plans = [r for r in (6, 7, 8, 9) if r < slots] + [slots]
    choice = choose(plans, groups, slots, trunc_steps)
    results = lax.switch(
        choice, [functools.partial(block_backward, n, groups, r, k) for k, r in enumerate(plans)],
        *args,
    )
    return tuple(emit(*results))


def solution(mesh):
    in_specs = (
        P("dp", "tensor", None),
        P("dp", "tensor", None),
        P(),
        P(),
        P(),
        P(),
        P(None, "tensor"),
        P(None, "tensor"),
        P(None, "tensor"),
    )
    out_specs = (
        P("dp", "tensor", None),
        P("dp", "tensor"),
        P("dp", "tensor"),
        P("dp", "tensor"),
        P(),
    )
    return jax.shard_map(
        per_device, mesh=mesh, in_specs=in_specs, out_specs=out_specs, check_vma=False
    )
```

```python
import functools

import jax
import jax.numpy as jnp
import numpy as np
from jax import lax
from jax.experimental import pallas as pl
from jax.experimental.pallas import tpu as pltpu
from jax.sharding import PartitionSpec as P

eps = 1e-05
early_round = 3


def noise_table():
    betas = np.linspace(0.00085**0.5, 0.012**0.5, 1000) ** 2
    abar = np.exp(np.cumsum(np.log1p(-betas)))
    return np.sqrt(1.0 - abar).astype(np.float32)


def pick(values, index):
    found = values[0]
    for k in range(1, len(values)):
        found = jnp.where(index == k, values[k], found)
    return found


def share(lives, rounds, early):
    over = [jnp.maximum(live - rounds, 0) for live in lives]
    near = [
        jnp.minimum(over[q], jnp.maximum(rounds - lives[q ^ 1], 0)) for q in range(len(lives))
    ]
    spare = [over[q] - near[q] for q in range(len(lives))]
    used = [jnp.minimum(live, rounds) + near[q ^ 1] for q, live in enumerate(lives)]
    begin = [jnp.maximum(u, early) for u in used]
    free = [rounds - b for b in begin]
    spare_at, free_at = [jnp.int32(0)], [jnp.int32(0)]
    for q in range(len(lives)):
        spare_at.append(spare_at[q] + spare[q])
        free_at.append(free_at[q] + free[q])
    return near, used, begin, spare_at, free_at


def block_kernel(n, groups, rounds, ahead, early, lag, late, steps_ref, times_ref, map_ref, table_ref, x_ref, cot_ref,
                 gain_ref, wv_hbm, wg_hbm, wo_hbm, ig_ref, gg_ref, dv_ref, dg_ref, do_ref,
                 full, part_a, part_b, in_a, in_b, sum_a, sum_b, last_a, last_b, held,
                 acc_v, acc_g, acc_o, placed, gain_one, gain_two,
                 dw_part, dw_pair, dw_sum, dw_down, dw_up, pool_near, pool_far, scale_ref, source_ref,
                 keep_ref, from_ref, near_ref, far_ref, item_ref,
                 ag_send, ag_recv, sa_send, sa_recv, sb_send, sb_recv, ta_send, ta_recv,
                 tb_send, tb_recv, out_send, out_recv, gain_send, gain_recv, far_send, far_recv,
                 pair_send, pair_recv, down_send, down_recv, up_send, up_recv,
                 pool_send, pool_recv, wv_ref, wg_ref, wo_ref, load_sem):
    slots, rows, width = x_ref.shape
    loads = [
        pltpu.make_async_copy(src, dst, load_sem.at[k])
        for k, (src, dst) in enumerate(((wv_hbm, wv_ref), (wg_hbm, wg_ref), (wo_hbm, wo_ref)))
    ]
    for copy in loads:
        copy.start()
    half = rows // 2
    extra = slots - rounds
    me = lax.axis_index("tensor")
    high = n // 2
    my_high, my_low = me // 2, me % 2
    pair = my_high * 2 + (1 - my_low)
    line_high = [(my_high + k) % high for k in range(1, high)]
    line = [h * 2 + my_low for h in line_high]
    peers = [(me + k) % n for k in range(1, n)]
    first = (((0,), (0,)), ((), ()))
    last = (((1,), (1,)), ((), ()))
    group = lax.axis_index("dp")
    chips = groups // 2
    chip, core = group // 2, group % 2
    twin = chip * 2 + (1 - core)
    block = dw_part.shape[2]
    mate = group + 2 - 4 * (chip % 2)
    base = group // 4 * 4
    lives = [jnp.clip(steps_ref[base + q] - 29, 1, slots) for q in range(4)]
    near, used, first_free, spare_at, free_at = share(lives, rounds, early)
    seat = group % 4
    own_live = pick(lives, seat)
    own_used = pick(used, seat)
    own_begin = pick(first_free, seat)
    own_free_at = pick(free_at[:4], seat)

    def cross(src, dst, send_sem, recv_sem, peer):
        return pltpu.make_async_remote_copy(
            src_ref=src, dst_ref=dst, send_sem=send_sem, recv_sem=recv_sem,
            device_id={"dp": peer}, device_id_type=pl.DeviceIdType.MESH,
        )

    def send(src, dst, send_sem, recv_sem, peer):
        return pltpu.make_async_remote_copy(
            src_ref=src, dst_ref=dst, send_sem=send_sem, recv_sem=recv_sem,
            device_id={"tensor": peer}, device_id_type=pl.DeviceIdType.MESH,
        )

    def out_copy(t, owner, index, peer):
        spot = placed.at[owner * rounds + t]
        return cross(spot, spot, out_send.at[t, index], out_recv.at[t, owner], peer)

    def own_outs(t, act):
        @pl.when(chip + 1 < chips)
        def _():
            act(out_copy(t, group, 0, group + 2))

        @pl.when(chip >= 1)
        def _():
            act(out_copy(t, group, 1, group - 2))

        act(out_copy(t, group, 2, twin))

    def relay_outs(t, d, act, arrive):
        base = 3 + 4 * (d - 1)

        @pl.when(chip >= d)
        def _():
            owner = group - 2 * d
            if arrive:
                out_copy(t, owner, base, twin).wait_recv()

            @pl.when(chip + 1 < chips)
            def _():
                act(out_copy(t, owner, base, group + 2))

            act(out_copy(t, owner, base + 1, twin))

        @pl.when(chip + d < chips)
        def _():
            owner = group + 2 * d
            if arrive:
                out_copy(t, owner, base + 2, twin).wait_recv()

            @pl.when(chip >= 1)
            def _():
                act(out_copy(t, owner, base + 2, group - 2))

            act(out_copy(t, owner, base + 3, twin))

    def begin(copy):
        copy.start()

    def done(copy):
        copy.wait_send()

    def own_copies(t):
        found = []
        for peer in [pair] + line:
            for kind in (0, 1):
                found.append(send(
                    full.at[t, kind, me], full.at[t, kind, me],
                    ag_send.at[t, len(found)], ag_recv.at[t, kind, me], peer,
                ))
        return found

    def passed_copies(t):
        found = []
        base = 2 * high
        for peer in line:
            found.append(send(
                full.at[t, 0, pair], full.at[t, 0, pair],
                ag_send.at[t, base + len(found)], ag_recv.at[t, 0, pair], peer,
            ))
        for owner in line:
            found.append(send(
                full.at[t, 1, owner], full.at[t, 1, owner],
                ag_send.at[t, base + len(found)], ag_recv.at[t, 1, owner], pair,
            ))
        return found

    def arrived(t, kind, owner):
        send(full.at[t, kind, owner], full.at[t, kind, owner], ag_send.at[t, 0],
             ag_recv.at[t, kind, owner], pair).wait_recv()

    def one_a(t):
        return [send(part_a.at[t, 1 - my_low], in_a.at[t], sa_send.at[t], sa_recv.at[t], pair)]

    def one_b(t):
        return [
            send(part_b.at[t, h], in_b.at[t, k], sb_send.at[t, k], sb_recv.at[t, k], p)
            for k, (h, p) in enumerate(zip(line_high, line, strict=True))
        ]

    def two_a(t):
        return [
            send(sum_a.at[t, k], last_a.at[t, k], ta_send.at[t, k], ta_recv.at[t, k], p)
            for k, p in enumerate(line)
        ]

    def two_b(t):
        return [send(sum_b.at[t], last_b.at[t], tb_send.at[t], tb_recv.at[t], pair)]

    def start_own(t):
        for copy in own_copies(t):
            copy.start()

    def pass_on(t):
        for owner in [pair] + line:
            for kind in (0, 1):
                arrived(t, kind, owner)
        for copy in passed_copies(t):
            copy.start()

    barrier = pltpu.get_barrier_semaphore()
    for peer in peers:
        pl.semaphore_signal(
            barrier, inc=1, device_id={"tensor": peer}, device_id_type=pl.DeviceIdType.MESH
        )
    for k in range(1, groups):
        pl.semaphore_signal(
            barrier, inc=1, device_id={"dp": (group + k) % groups},
            device_id_type=pl.DeviceIdType.MESH,
        )
    for kind, ref in enumerate((x_ref, cot_ref)):
        full[0, kind, me] = ref[0]
    pl.semaphore_wait(barrier, n - 1 + groups - 1)
    locals_ = (x_ref, cot_ref) if extra else ()
    near_copies = [
        cross(ref.at[pl.ds(rounds, extra)], pool_near.at[kind], pool_send.at[kind, 0],
              pool_recv.at[kind, 0], twin)
        for kind, ref in enumerate(locals_)
    ]
    far_pool = [
        cross(ref.at[pl.ds(rounds, extra)], pool_far.at[kind, pl.ds(0, extra)],
              pool_send.at[kind, 1], pool_recv.at[kind, 1], mate)
        for kind, ref in enumerate(locals_)
    ]
    far_passed = [
        cross(pool_far.at[kind, pl.ds(0, extra)], pool_far.at[kind, pl.ds(extra, extra)],
              pool_send.at[kind, 2], pool_recv.at[kind, 2], twin)
        for kind, ref in enumerate(locals_)
    ]
    start_own(0)
    for copy in near_copies + far_pool:
        copy.start()

    def set_scale(t, carry):
        mine = t < own_live
        beside = t < own_used
        order = own_free_at + t - own_begin
        item = base * slots
        away_at = jnp.int32(0)
        for q in range(4):
            inside = jnp.logical_and(order >= spare_at[q], order < spare_at[q + 1])
            k = near[q] + order - spare_at[q]
            item = jnp.where(inside, (base + q) * slots + rounds + k, item)
            away_at = jnp.where(inside, jnp.where(core == q % 2, 0, extra) + k, away_at)
        item = jnp.where(beside, twin * slots + rounds + t - own_live, item)
        item = jnp.where(mine, group * slots + t, item)
        item = jnp.clip(item, 0, groups * slots - 1)
        distant = jnp.logical_and(t >= own_begin, order < spare_at[4])
        alive = jnp.logical_or(beside, distant)
        scale_ref[t] = jnp.where(alive, table_ref[times_ref[item]], 0.0)
        from_ref[t] = jnp.where(mine, 0, jnp.where(beside, 1, 2))
        near_ref[t] = jnp.clip(t - own_live, 0, max(extra - 1, 0))
        far_ref[t] = jnp.clip(away_at, 0, max(2 * extra - 1, 0))
        return carry

    lax.fori_loop(0, rounds, set_scale, 0)
    for copy in near_copies:
        copy.wait()

    def fill(t, carry):
        for kind, ref in enumerate((x_ref, cot_ref)):
            tile = ref[t]
            if extra:
                tile = jnp.where(from_ref[t] == 0, tile, pool_near[kind, near_ref[t]])
            full[t, kind, me] = tile
        return carry

    def fill_late(t, carry):
        for kind, ref in enumerate((x_ref, cot_ref)):
            tile = jnp.where(from_ref[t] == 0, ref[t], pool_near[kind, near_ref[t]])
            full[t, kind, me] = jnp.where(from_ref[t] == 2, pool_far[kind, far_ref[t]], tile)
        return carry

    lax.fori_loop(1, early if extra else rounds, fill, 0)
    started = min(ahead + 1, early if extra else rounds)
    for t in range(1, started):
        start_own(t)

    def invert(i, found):
        spot = map_ref[i] - group * slots
        return tuple(jnp.where(spot == s, i, item) for s, item in enumerate(found))

    items = lax.fori_loop(0, groups * slots, invert, tuple(jnp.int32(0) for _ in range(slots)))
    for s, item in enumerate(items):
        item_ref[s] = item

    def locate(s, carry):
        item = item_ref[s]
        owner = item // slots
        index = item % slots
        root = owner // 4 * 4
        place_in = owner - root
        there = [jnp.clip(steps_ref[root + q] - 29, 1, slots) for q in range(4)]
        near, used, first_free, spare_at, free_at = share(there, rounds, early)
        other = owner + 1 - 2 * (owner % 2)
        own_near = pick(near, place_in)
        order = pick(spare_at[:4], place_in) + index - rounds - own_near
        spot = jnp.int32(0)
        for q in range(4):
            inside = jnp.logical_and(order >= free_at[q], order < free_at[q + 1])
            spot = jnp.where(
                inside, (root + q) * rounds + first_free[q] + order - free_at[q], spot
            )
        beside = other * rounds + pick([there[q ^ 1] for q in range(4)], place_in) + index - rounds
        spot = jnp.where(index < rounds + own_near, beside, spot)
        spot = jnp.where(index < rounds, owner * rounds + index, spot)
        source_ref[s] = jnp.clip(spot, 0, groups * rounds - 1)
        keep_ref[s] = jnp.where(index < pick(there, place_in), 1.0, 0.0)
        return carry

    lax.fori_loop(0, slots, locate, 0)

    inner = acc_v.shape[1]

    def clear(d, carry):
        for acc in (acc_v, acc_g, acc_o):
            acc[pl.ds(pl.multiple_of(d * block, 8), block), :] = jnp.zeros(
                (block, inner), jnp.float32
            )
        return carry

    lax.fori_loop(0, groups, clear, 0)
    gg_ref[...] = jnp.zeros_like(gg_ref)
    gain = gain_ref[...].reshape(1, width)
    pass_on(0)
    for copy in loads:
        copy.wait()

    def combine(t):
        for copy in one_a(t):
            copy.wait_recv()
        sums = []
        for h in range(high):
            mine = pick([part_a[t, l, h] for l in range(2)], my_low)
            sums.append(mine.astype(jnp.float32) + in_a[t, h].astype(jnp.float32))
        for k, h in enumerate(line_high):
            sum_a[t, k] = pick(sums, h).astype(jnp.bfloat16)
        for copy in two_a(t):
            copy.start()
        held[t, 0] = pick(sums, my_high)
        for copy in one_b(t):
            copy.wait_recv()
        sums = []
        for l in range(2):
            both = pick([part_b[t, h, l] for h in range(high)], my_high).astype(jnp.float32)
            for k in range(high - 1):
                both += in_b[t, k, l].astype(jnp.float32)
            sums.append(both)
        sum_b[t] = pick(sums, 1 - my_low).astype(jnp.bfloat16)
        for copy in two_b(t):
            copy.start()
        held[t, 1] = pick(sums, my_low)

    def finish(t):
        top = held[t, 0]
        low = held[t, 1]
        for k, copy in enumerate(two_a(t)):
            copy.wait_recv()
            top += last_a[t, k].astype(jnp.float32)
        for copy in two_b(t):
            copy.wait_recv()
        low += last_b[t].astype(jnp.float32)
        d_normed = jnp.concatenate([top, low], axis=0)
        x = full[t, 0, me].astype(jnp.float32)
        centred = x - jnp.mean(x, axis=-1, keepdims=True)
        inv_std = lax.rsqrt(jnp.mean(centred * centred, axis=-1, keepdims=True) + eps)
        x_hat = centred * inv_std
        grad = (full[t, 1, me].astype(jnp.float32) * scale_ref[t]).astype(jnp.bfloat16)
        d_hat = d_normed * gain
        placed[group * rounds + t] = (grad.astype(jnp.float32) + inv_std * (
            d_hat
            - jnp.mean(d_hat, axis=-1, keepdims=True)
            - x_hat * jnp.mean(d_hat * x_hat, axis=-1, keepdims=True)
        )).astype(jnp.bfloat16)
        own_outs(t, begin)
        gg_ref[...] += jnp.sum(d_normed * x_hat, axis=0, keepdims=True)

    def after(t):
        @pl.when(t >= lag)
        def _():
            combine(t - lag)

        @pl.when(t >= late)
        def _():
            finish(t - late)

        for d in range(1, chips):
            @pl.when(t >= late + d)
            def _():
                relay_outs(t - late - d, d, begin, True)

    def relay_left(t):
        for d in range(1, chips):
            if 0 <= t - late - d < rounds:
                relay_outs(t - late - d, d, begin, True)

    def one_tile(t, carry):
        @pl.when(t == 1)
        def _():
            if extra:
                for copy in far_passed:
                    copy.wait_recv()
                lax.fori_loop(early, rounds, fill_late, 0)
            for later in range(started, min(ahead + 2, rounds)):
                start_own(later)

        @pl.when(t >= 2)
        def _():
            @pl.when(t + ahead < rounds)
            def _():
                start_own(t + ahead)

        @pl.when(t + 1 < rounds)
        def _():
            pass_on(t + 1)

        far = [h * 2 + (1 - my_low) for h in line_high]
        for owner in far:
            for kind in (0, 1):
                arrived(t, kind, owner)
        x = full[t, 0].reshape(n * rows, width).astype(jnp.float32)
        centred = x - jnp.mean(x, axis=-1, keepdims=True)
        inv_std = lax.rsqrt(jnp.mean(centred * centred, axis=-1, keepdims=True) + eps)
        normed = (centred * inv_std * gain).astype(jnp.bfloat16)
        cot = full[t, 1].reshape(n * rows, width).astype(jnp.float32)
        grad = (cot * scale_ref[t]).astype(jnp.bfloat16)
        values = jnp.dot(normed, wv_ref[...], preferred_element_type=jnp.float32)
        gate = jnp.dot(normed, wg_ref[...], preferred_element_type=jnp.float32)
        d_hidden = jnp.dot(grad, wo_ref[...], preferred_element_type=jnp.float32)
        cdf = 0.5 * (1.0 + lax.erf(gate * 0.7071067811865476))
        density = jnp.exp(-0.5 * gate * gate) * 0.3989422804014327
        gelu = gate * cdf
        hidden = (values * gelu).astype(jnp.bfloat16)
        d_value = (d_hidden * gelu).astype(jnp.bfloat16)
        d_gate = (d_hidden * values * (cdf + gate * density)).astype(jnp.bfloat16)
        d_normed = lax.dot_general(d_value, wv_ref[...], last, preferred_element_type=jnp.float32)
        d_normed += lax.dot_general(d_gate, wg_ref[...], last, preferred_element_type=jnp.float32)
        d_normed = d_normed.astype(jnp.bfloat16).reshape(n, rows, width)
        for h in range(high):
            for l in range(2):
                part_a[t, l, h] = d_normed[h * 2 + l, :half]
                part_b[t, h, l] = d_normed[h * 2 + l, half:]
        for copy in one_a(t) + one_b(t):
            copy.start()
        acc_v[...] += lax.dot_general(normed, d_value, first, preferred_element_type=jnp.float32)
        acc_g[...] += lax.dot_general(normed, d_gate, first, preferred_element_type=jnp.float32)
        acc_o[...] += lax.dot_general(grad, hidden, first, preferred_element_type=jnp.float32)
        if extra:
            @pl.when(t == 0)
            def _():
                for copy in far_pool:
                    copy.wait_recv()
                for copy in far_passed:
                    copy.start()

        after(t)
        return carry

    lax.fori_loop(0, rounds, one_tile, 0)
    pair_copies = [
        cross(dw_part.at[c * 2 + 1 - core], dw_pair.at[c], pair_send.at[c], pair_recv.at[c], twin)
        for c in range(chips)
    ]

    def narrow(d, carry):
        for k, acc in enumerate((acc_v, acc_g, acc_o)):
            part = acc[pl.ds(pl.multiple_of(d * block, 8), block), :]
            dw_part[d, k] = part.astype(jnp.bfloat16)
        return carry

    ready = []
    for j in range(chips - 1):
        for c in (j, chips - 1 - j):
            if c not in ready:
                ready.append(c)
                lax.fori_loop(2 * c, 2 * c + 2, narrow, 0)
                pair_copies[c].start()
    for t in range(rounds, rounds + late - 1):
        if t - lag < rounds:
            combine(t - lag)
        if t >= late:
            finish(t - late)
        relay_left(t)

    def down_copy(c, k):
        return cross(dw_sum.at[c, k], dw_down.at[c, k], down_send.at[c, k], down_recv.at[c, k],
                     group - 2)

    def up_copy(c, k):
        return cross(dw_sum.at[c, k], dw_up.at[c, k], up_send.at[c, k], up_recv.at[c, k], group + 2)

    def move(j, k):
        c = chips - 1 - j

        @pl.when(chip > j)
        def _():
            @pl.when(chip + 1 < chips)
            def _():
                down_copy(j, k).wait_recv()
                both = dw_sum[j, k].astype(jnp.float32) + dw_down[j, k].astype(jnp.float32)
                dw_sum[j, k] = both.astype(jnp.bfloat16)
                down_copy(j, k).start()

        @pl.when(chip < c)
        def _():
            @pl.when(chip >= 1)
            def _():
                up_copy(c, k).wait_recv()
                both = dw_sum[c, k].astype(jnp.float32) + dw_up[c, k].astype(jnp.float32)
                dw_sum[c, k] = both.astype(jnp.bfloat16)
                up_copy(c, k).start()

    gain_copies = [
        send(gg_ref, gain_one.at[me], gain_send.at[k], gain_recv.at[me], peer)
        for k, peer in enumerate(peers)
    ]
    for c in ready:
        pair_copies[c].wait()
        both = dw_part[c * 2 + core].astype(jnp.float32) + dw_pair[c].astype(jnp.float32)
        dw_sum[c] = both.astype(jnp.bfloat16)
    finish(rounds - 1)
    parts = [(j, k) for j in range(chips - 1) for k in range(3)]
    for j, k in parts:
        @pl.when(chip == chips - 1)
        def _():
            down_copy(j, k).start()

        @pl.when(chip == 0)
        def _():
            up_copy(chips - 1 - j, k).start()

    relay_left(rounds + late - 1)
    gain_one[me] = gg_ref[...]
    for copy in gain_copies:
        copy.start()
    far_copies = [
        cross(gain_two.at[group], gain_two.at[group], far_send.at[k], far_recv.at[group],
              (group + k) % groups)
        for k in range(1, groups)
    ]

    def share_gain():
        for peer in peers:
            send(gg_ref, gain_one.at[peer], gain_send.at[0], gain_recv.at[peer], peer).wait_recv()
        for copy in gain_copies:
            copy.wait_send()
        gain_sum = gain_one[0]
        for k in range(1, n):
            gain_sum += gain_one[k]
        gain_two[group] = gain_sum
        for copy in far_copies:
            copy.start()

    left = list(range(rounds + late, rounds + late - 1 + chips))
    for index, (j, k) in enumerate(parts):
        if index != 1 and left:
            relay_left(left.pop(0))
        if index == 1:
            share_gain()
        move(j, k)
    for t in left:
        relay_left(t)
    def settle(t, carry):
        for c in range(chips):
            out_copy(t, c * 2 + 1 - core, 0, twin).wait_recv()
        for copy in (own_copies(t) + passed_copies(t) + one_a(t) + one_b(t) + two_a(t) + two_b(t)):
            copy.wait_send()
        own_outs(t, done)
        for d in range(1, chips):
            relay_outs(t, d, done, False)
        return carry

    lax.fori_loop(0, rounds, settle, 0)
    for copy in far_pool + far_passed:
        copy.wait_send()

    def place(t, carry):
        ig_ref[t] = (placed[source_ref[t]].astype(jnp.float32) * keep_ref[t]).astype(jnp.bfloat16)
        return carry

    lax.fori_loop(0, slots, place, 0)
    for k in range(1, groups):
        peer = (group + k) % groups
        cross(gain_two.at[peer], gain_two.at[peer], far_send.at[k], far_recv.at[peer],
              peer).wait_recv()
    for copy in far_copies:
        copy.wait_send()
    gain_total = gain_two[0]
    for k in range(1, groups):
        gain_total += gain_two[k]
    gg_ref[...] = gain_total
    outs = (dv_ref, dg_ref, do_ref)
    for c in range(chips):
        @pl.when(chip == c)
        def _():
            for k, ref in enumerate(outs):
                total = dw_sum[c, k].astype(jnp.float32)
                if c + 1 < chips:
                    down_copy(c, k).wait_recv()
                    total += dw_down[c, k].astype(jnp.float32)
                if c >= 1:
                    up_copy(c, k).wait_recv()
                    total += dw_up[c, k].astype(jnp.float32)
                ref[...] = total

    for j in range(chips - 1):
        for k in range(3):
            @pl.when(chip > j)
            def _():
                down_copy(j, k).wait_send()

            @pl.when(chip < chips - 1 - j)
            def _():
                up_copy(chips - 1 - j, k).wait_send()


def block_backward(n, groups, rounds, ident, steps, times, tile_map, table, x, cot, gain,
                   w_value, w_gate, w_out):
    slots, rows, width = x.shape
    inner = w_value.shape[1]
    chips = groups // 2
    high = n // 2
    half = rows // 2
    others = max(high - 1, 1)
    block = width // groups
    vmem = pl.BlockSpec(memory_space=pltpu.VMEM)
    smem = pl.BlockSpec(memory_space=pltpu.SMEM)
    grads = jax.ShapeDtypeStruct((block, inner), jnp.float32)
    dma = pltpu.SemaphoreType.DMA
    bf16 = jnp.bfloat16
    return pl.pallas_call(
        functools.partial(block_kernel, n, groups, rounds, 2, min(early_round, rounds), 1, 2),
        in_specs=[smem] * 4 + [vmem] * 3 + [pl.BlockSpec(memory_space=pltpu.HBM)] * 3,
        out_specs=[vmem] * 5,
        out_shape=[
            jax.ShapeDtypeStruct((slots, rows, width), bf16),
            jax.ShapeDtypeStruct((1, width), jnp.float32),
            grads,
            grads,
            grads,
        ],
        scratch_shapes=[
            pltpu.VMEM((rounds, 2, n, rows, width), bf16),
            pltpu.VMEM((rounds, 2, high, half, width), bf16),
            pltpu.VMEM((rounds, high, 2, half, width), bf16),
            pltpu.VMEM((rounds, high, half, width), bf16),
            pltpu.VMEM((rounds, others, 2, half, width), bf16),
            pltpu.VMEM((rounds, others, half, width), bf16),
            pltpu.VMEM((rounds, half, width), bf16),
            pltpu.VMEM((rounds, others, half, width), bf16),
            pltpu.VMEM((rounds, half, width), bf16),
            pltpu.VMEM((rounds, 2, half, width), jnp.float32),
        ]
        + [pltpu.VMEM((width, inner), jnp.float32)] * 3
        + [
            pltpu.VMEM((groups * rounds, rows, width), bf16),
            pltpu.VMEM((n, 1, width), jnp.float32),
            pltpu.VMEM((groups, 1, width), jnp.float32),
            pltpu.VMEM((groups, 3, block, inner), bf16),
            pltpu.VMEM((chips, 3, block, inner), bf16),
            pltpu.VMEM((chips, 3, block, inner), bf16),
            pltpu.VMEM((chips, 3, block, inner), bf16),
            pltpu.VMEM((chips, 3, block, inner), bf16),
            pltpu.VMEM((2, max(slots - rounds, 1), rows, width), bf16),
            pltpu.VMEM((2, max(2 * (slots - rounds), 1), rows, width), bf16),
            pltpu.SMEM((rounds,), jnp.float32),
            pltpu.SMEM((slots,), jnp.int32),
            pltpu.SMEM((slots,), jnp.float32),
            pltpu.SMEM((rounds,), jnp.int32),
            pltpu.SMEM((rounds,), jnp.int32),
            pltpu.SMEM((rounds,), jnp.int32),
            pltpu.SMEM((slots,), jnp.int32),
            dma((rounds, n + 2 * (high - 1))),
            dma((rounds, 2, n)),
            dma((rounds,)),
            dma((rounds,)),
            dma((rounds, high)),
            dma((rounds, high)),
            dma((rounds, high)),
            dma((rounds, high)),
            dma((rounds,)),
            dma((rounds,)),
            dma((rounds, 3 + 4 * (chips - 1))),
            dma((rounds, groups)),
            dma((n,)),
            dma((n,)),
            dma((groups,)),
            dma((groups,)),
            dma((chips,)),
            dma((chips,)),
            dma((chips, 3)),
            dma((chips, 3)),
            dma((chips, 3)),
            dma((chips, 3)),
            dma((2, 3)),
            dma((2, 3)),
        ]
        + [pltpu.VMEM((width, inner), bf16)] * 3
        + [
            dma((3,)),
        ],
        compiler_params=pltpu.CompilerParams(
            collective_id=ident, has_side_effects=True, vmem_limit_bytes=60 * 1024 * 1024
        ),
    )(steps, times, tile_map, table, x, cot, gain, w_value, w_gate, w_out)


def emit_kernel(ig_ref, gg_ref, dv_ref, dg_ref, do_ref, a_ref, b_ref, c_ref, d_ref, e_ref):
    a_ref[...] = ig_ref[...]
    b_ref[...] = dv_ref[...]
    c_ref[...] = dg_ref[...]
    d_ref[...] = do_ref[...]
    e_ref[...] = gg_ref[0, :]


def emit(ig, gg, dv, dg, do):
    vmem = pl.BlockSpec(memory_space=pltpu.VMEM)
    outs = [jax.ShapeDtypeStruct(a.shape, a.dtype) for a in (ig, dv, dg, do)]
    outs.append(jax.ShapeDtypeStruct((gg.shape[1],), gg.dtype))
    return pl.pallas_call(
        emit_kernel, in_specs=[vmem] * 5, out_specs=[vmem] * 5, out_shape=outs,
    )(ig, gg, dv, dg, do)


def choose_kernel(plans, groups, slots, steps_ref, choice_ref):
    choice = jnp.int32(0)
    blocked = jnp.int32(1)
    for rounds in plans[:-1]:
        lacking = jnp.int32(0)
        for base in range(0, groups, 4):
            lives = [jnp.clip(steps_ref[base + q] - 29, 1, slots) for q in range(4)]
            _, _, _, spare_at, free_at = share(lives, rounds, min(early_round, rounds))
            lacking = jnp.maximum(lacking, spare_at[4] - free_at[4])
        blocked = jnp.where(lacking > 0, blocked, 0)
        choice = choice + blocked
    choice_ref[0] = choice


def choose(plans, groups, slots, steps):
    smem = pl.BlockSpec(memory_space=pltpu.SMEM)
    return pl.pallas_call(
        functools.partial(choose_kernel, plans, groups, slots), in_specs=[smem], out_specs=smem,
        out_shape=jax.ShapeDtypeStruct((1,), jnp.int32),
    )(steps)[0]


def per_device(latents, cotangent, trunc_steps, timesteps, tile_map, gain, w_value, w_gate, w_out):
    slots = latents.shape[0]
    n, groups = lax.axis_size("tensor"), lax.axis_size("dp")
    table = jnp.asarray(noise_table())
    args = (trunc_steps, timesteps, tile_map, table, latents, cotangent, gain, w_value, w_gate, w_out)
    plans = [r for r in (6, 7, 8) if r < slots] + [slots]
    choice = choose(plans, groups, slots, trunc_steps)
    results = lax.switch(
        choice, [functools.partial(block_backward, n, groups, r, k) for k, r in enumerate(plans)],
        *args,
    )
    return tuple(emit(*results))


def solution(mesh):
    in_specs = (
        P("dp", "tensor", None),
        P("dp", "tensor", None),
        P(),
        P(),
        P(),
        P(),
        P(None, "tensor"),
        P(None, "tensor"),
        P(None, "tensor"),
    )
    out_specs = (
        P("dp", "tensor", None),
        P("dp", "tensor"),
        P("dp", "tensor"),
        P("dp", "tensor"),
        P(),
    )
    return jax.shard_map(
        per_device, mesh=mesh, in_specs=in_specs, out_specs=out_specs, check_vma=False
    )
```
